128 devices in a mesh: gx: 8 (over y, x_lo), pa: 16 (over x_hi, z, core).
Axes of the slice: x: 4 (x_hi: 2, x_lo: 2; x = x_hi * 2 + x_lo), y: 4, z: 4, core: 2. Of those that a mesh axis runs over, the one named last changes fastest.
Arguments:
- plastic: float32 [6, 128, 128, 128], P(None, 'gx', 'pa'), may hold values from -6 to 6
- offsets: float32 [3, 16, 32, 128], P(None, 'pa', 'gx'), may hold values from 0 to 1
- lines: float32 [3, 16, 32, 128], P(None, 'pa', 'gx'), may hold values from -3 to 3
- burgers: float32 [3, 16, 32, 128], P(None, 'pa', 'gx'), may hold values from -3.6 to 3.6
- counts: int32 [16, 32], P('pa', 'gx'), may hold values from 1 to 128, as said below
- voxels: int32 [16, 32, 128], P('pa', 'gx'), may hold values from 0 to 16383, as said below
Outputs:
- stress: float32 [6, 128, 128, 128], P(None, 'gx', 'pa')
- moved: float32 [3, 16, 32, 128], P(None, 'pa', 'gx')
The draws below stay inside these ranges and needn't reach their ends.
Inputs may be any that keep to these rules, and one draw needn't show every extreme that they name: `counts`: each count is at least 1 and some cell holds 128 live segments. `voxels`: A segment of cell c lies in its device's block of 16 x 8 x 128 grid points: v = (x * 8 + y) * 128 + z with local plane x among the 4 planes of cell c % 4.
All inputs are finite; a program needn't handle non-finite values.
Results may differ from the reference program's by a relative error of at most 0.0003.
Values sent between devices are 32-bit elements; how exact they have to be, the bound alone decides.
A program may use at most 64 MiB of HBM per device.

```python
import math
import jax
import jax.numpy as jnp
from jax import lax

GRID = 128
CELLS_DEV = 4
CAP = 128
SUB = 3
CELLS = 32
SLABS = 16
XL = 16
YL = 8


def draw_counts(key, part):
    first_key, second_key = jax.random.split(key)
    raw_count = jax.random.randint(first_key, (SLABS, CELLS // CELLS_DEV, CELLS_DEV), 1, CAP + 1)
    load_level = jax.random.randint(second_key, (SLABS, CELLS // CELLS_DEV, 1), 1, 5)
    scaled = jnp.maximum(1, raw_count * load_level // 4).reshape(SLABS, CELLS)
    return scaled.at[0, 0].set(CAP).astype(jnp.int32)


def draw_voxels(key, part):
    subkeys = jax.random.split(key, 3)
    per_cell = XL // CELLS_DEV
    cell_local = (jnp.arange(CELLS, dtype=jnp.int32) % CELLS_DEV)[None, :, None]
    pick_x = jax.random.randint(subkeys[0], (SLABS, CELLS, CAP), 0, per_cell)
    pick_y = jax.random.randint(subkeys[1], (SLABS, CELLS, CAP), 0, YL)
    pick_z = jax.random.randint(subkeys[2], (SLABS, CELLS, CAP), 0, GRID)
    return (((cell_local * per_cell + pick_x) * YL + pick_y) * GRID + pick_z).astype(jnp.int32)


def levels(stream_key, shape, pieces, least, largest):
    def one(dim, parts):
        heights = jax.random.uniform(jax.random.fold_in(jax.random.fold_in(stream_key, 6), dim), (parts,), jnp.float32, least / len(pieces), largest / len(pieces))
        return jnp.repeat(jnp.exp(heights), shape[dim] // parts).reshape((-1,) + (1,) * (len(shape) - dim - 1))

    factor_of = one(*pieces[0])
    for cut in pieces[1:]:
        factor_of = factor_of * one(*cut)
    return factor_of


def gaussian(stream_key, extent, deviation, limit, shards=(), kind=jnp.bfloat16):
    values = jax.random.normal(stream_key, extent, jnp.float32) * deviation
    if len(shards) > 0:
        values = levels(stream_key, extent, shards, -0.22, 0.18) * values
    return jnp.clip(values, min=-limit, max=limit).astype(kind)


def setup_inputs(seed: int = 0) -> dict:
    key_of = jax.random.split(jax.random.key(seed), 7)
    return {
        "plastic": gaussian(key_of[0], (6, GRID, GRID, GRID), 1.0, 6.0, ((1, 8), (2, 16)), jnp.float32),
        "offsets": jnp.clip(1.0 * jax.random.uniform(key_of[1], (3, SLABS, CELLS, CAP), jnp.float32) ** levels(key_of[1], (3, SLABS, CELLS, CAP), ((1, 16), (2, 8)), -0.2, 0.2), 0.0, 1.0),
        "lines": gaussian(key_of[2], (3, SLABS, CELLS, CAP), 0.5, 3.0, ((1, 16), (2, 8)), jnp.float32),
        "burgers": gaussian(key_of[3], (3, SLABS, CELLS, CAP), 0.6, 3.6, ((1, 16), (2, 8)), jnp.float32),
        "counts": draw_counts(jax.random.fold_in(key_of[6], 71), 0),
        "voxels": draw_voxels(jax.random.fold_in(key_of[6], 71), 0),
    }


lame_lambda = 1.5
shear_modulus = 1.0
green_coef = 2.5 / 3.5
core_square = 0.09
pair_factor = 1.0 / (4.0 * math.pi)
step_size = 0.05
full_index = ((0, 5, 4), (5, 1, 3), (4, 3, 2))

def stress_of(strain, freq_x, freq_y, freq_z):
    strain_xx, strain_yy, strain_zz = (strain[0], strain[1], strain[2])
    strain_yz, strain_xz, strain_xy = (strain[3], strain[4], strain[5])
    trace = strain_xx + strain_yy + strain_zz
    tau_xx = lame_lambda * trace + 2.0 * shear_modulus * strain_xx
    tau_yy = lame_lambda * trace + 2.0 * shear_modulus * strain_yy
    tau_zz = lame_lambda * trace + 2.0 * shear_modulus * strain_zz
    tau_yz = 2.0 * shear_modulus * strain_yz
    tau_xz = 2.0 * shear_modulus * strain_xz
    tau_xy = 2.0 * shear_modulus * strain_xy
    norm_x = tau_xx * freq_x + tau_xy * freq_y + tau_xz * freq_z
    norm_y = tau_xy * freq_x + tau_yy * freq_y + tau_yz * freq_z
    norm_z = tau_xz * freq_x + tau_yz * freq_y + tau_zz * freq_z
    square = freq_x * freq_x + freq_y * freq_y + freq_z * freq_z
    inverse = 1.0 / jnp.maximum(square, 1.0)
    along_k = (freq_x * norm_x + freq_y * norm_y + freq_z * norm_z) * inverse * inverse * green_coef

    def strain_term(first_q, second_q, first_n, second_n, plastic_part):
        total = (first_q * second_n + second_q * first_n) * inverse / (2.0 * shear_modulus) - first_q * second_q * along_k
        return total - plastic_part
    el_xx = strain_term(freq_x, freq_x, norm_x, norm_x, strain_xx)
    el_yy = strain_term(freq_y, freq_y, norm_y, norm_y, strain_yy)
    el_zz = strain_term(freq_z, freq_z, norm_z, norm_z, strain_zz)
    el_yz = strain_term(freq_y, freq_z, norm_y, norm_z, strain_yz)
    el_xz = strain_term(freq_x, freq_z, norm_x, norm_z, strain_xz)
    el_xy = strain_term(freq_x, freq_y, norm_x, norm_y, strain_xy)
    el_trace = el_xx + el_yy + el_zz
    return jnp.stack([lame_lambda * el_trace + 2.0 * shear_modulus * el_xx, lame_lambda * el_trace + 2.0 * shear_modulus * el_yy, lame_lambda * el_trace + 2.0 * shear_modulus * el_zz, 2.0 * shear_modulus * el_yz, 2.0 * shear_modulus * el_xz, 2.0 * shear_modulus * el_xy])

def advance(position, lines, burgers, sampled):
    cell_count = sampled.shape[1]
    unit_x = jnp.array([1.0, 0.0, 0.0], jnp.float32)[:, None, None]
    source = jnp.concatenate([position[:, shifted:shifted + cell_count] + (shifted - 1.0) * unit_x for shifted in range(3)], axis=2)
    source_line = jnp.concatenate([lines[:, shifted:shifted + cell_count] for shifted in range(3)], axis=2)
    source_burgers = jnp.concatenate([burgers[:, shifted:shifted + cell_count] for shifted in range(3)], axis=2)
    target = position[:, 1:cell_count + 1]
    own_line = lines[:, 1:cell_count + 1]
    own_burgers = burgers[:, 1:cell_count + 1]
    offset_vec = target[:, :, :, None] - source[:, :, None, :]
    radius = offset_vec[0] ** 2 + offset_vec[1] ** 2 + offset_vec[2] ** 2 + core_square
    weight = lax.rsqrt(radius) / radius
    line_b = source_line[:, :, None, :]
    cross = jnp.stack([offset_vec[1] * line_b[2] - offset_vec[2] * line_b[1], offset_vec[2] * line_b[0] - offset_vec[0] * line_b[2], offset_vec[0] * line_b[1] - offset_vec[1] * line_b[0]]) * weight[None]
    moment = jnp.einsum('acij,bcj->abci', cross, source_burgers, precision=lax.Precision.HIGHEST)
    pair_field = pair_factor * (moment + jnp.swapaxes(moment, 0, 1))
    traction = []
    for first in range(3):
        acc_row = jnp.zeros_like(target[0])
        for second in range(3):
            acc_row = acc_row + (sampled[full_index[first][second]] + pair_field[first, second]) * own_burgers[second]
        traction.append(acc_row)
    force_x = traction[1] * own_line[2] - traction[2] * own_line[1]
    force_y = traction[2] * own_line[0] - traction[0] * own_line[2]
    force_z = traction[0] * own_line[1] - traction[1] * own_line[0]
    return target + step_size * jnp.stack([force_x, force_y, force_z])

def extend(array):
    return jnp.concatenate([array[:, -1:], array, array[:, :1]], axis=1)

def reference(plastic, offsets, lines, burgers, counts, voxels):
    spectrum = jnp.fft.rfftn(plastic, axes=(1, 2, 3))
    grid_index = jnp.arange(GRID, dtype=jnp.int32)
    signed = jnp.where(grid_index < GRID // 2, grid_index, jnp.where(grid_index == GRID // 2, 0, grid_index - GRID)).astype(jnp.float32)
    half_index = jnp.arange(GRID // 2 + 1, dtype=jnp.int32)
    half_freq = jnp.where(half_index < GRID // 2, half_index, 0).astype(jnp.float32)
    freq_x = signed[:, None, None]
    freq_y = signed[None, :, None]
    freq_z = half_freq[None, None, :]
    real_part = stress_of(jnp.real(spectrum), freq_x, freq_y, freq_z)
    imag_part = stress_of(jnp.imag(spectrum), freq_x, freq_y, freq_z)
    stress_spectrum = lax.complex(real_part, imag_part)
    stress = jnp.fft.irfftn(stress_spectrum, s=(GRID, GRID, GRID), axes=(1, 2, 3)).astype(jnp.float32)
    live_mask = (jnp.arange(CAP, dtype=jnp.int32)[None, None, :] < counts[:, :, None]).astype(jnp.float32)
    masked = burgers * live_mask[None]
    local_x = voxels // (YL * GRID)
    remain = voxels % (YL * GRID)
    local_y = remain // GRID
    local_z = remain % GRID
    owner_gx = (jnp.arange(CELLS, dtype=jnp.int32) // CELLS_DEV)[None, :, None]
    slab_index = jnp.arange(SLABS, dtype=jnp.int32)[:, None, None]
    grid_x = (owner_gx * XL + local_x).astype(jnp.int32)
    grid_y = (slab_index * YL + local_y).astype(jnp.int32)
    sampled = stress[:, grid_x, grid_y, local_z.astype(jnp.int32)]

    def per_slab(items):
        initial, line_dirs, burg_dirs, sample_slab = items
        position = initial
        for repeat in range(SUB):
            position = advance(extend(position), extend(line_dirs), extend(burg_dirs), sample_slab)
        return position - initial
    moved = lax.map(per_slab, (jnp.moveaxis(offsets, 1, 0), jnp.moveaxis(lines, 1, 0), jnp.moveaxis(masked, 1, 0), jnp.moveaxis(sampled, 1, 0)))
    return (stress, jnp.moveaxis(moved, 0, 1))
```

```python
import math

import jax
import jax.numpy as jnp
import numpy as np
from jax import lax
from jax.experimental import pallas as pl
from jax.experimental.pallas import tpu as pltpu
from jax.sharding import PartitionSpec as P

MESH = pl.DeviceIdType.MESH
F32 = jnp.float32
BF16 = jnp.bfloat16
N = 128
SLOTS = 32
CHUNKS = 3
CELLS = 4
HALO = 3
WIDE = CELLS + 2 * HALO

lame_lambda = 1.5
shear_modulus = 1.0
green_coef = 2.5 / 3.5
core_square = 0.09
pair_factor = 1.0 / (4.0 * math.pi)
step_size = 0.05
full_index = ((0, 5, 4), (5, 1, 3), (4, 3, 2))


def split_table(table):
    table = jnp.asarray(table, F32)
    high = table.astype(BF16)
    low = (table - high.astype(F32)).astype(BF16)
    return high, low


def np_split(table):
    table = np.asarray(table, np.float32)
    high = table.astype(jnp.bfloat16)
    low = (table - high.astype(np.float32)).astype(jnp.bfloat16)
    return high, low


def tables():
    index = np.arange(N)
    angle = 2.0 * np.pi * (np.outer(index, index) % N) / N
    cos, sin = np.cos(angle), np.sin(angle)
    lane = np.arange(N)
    bins = (lane // 4) * 2 + lane % 2
    part = (lane // 2) % 2
    ahead_z = np.where(part[None, :] == 0, cos[:, bins], -sin[:, bins])
    ahead_z = np.where((bins == 0)[None, :] & (part == 1)[None, :], cos[:, 64][:, None], ahead_z)
    weight = np.where(bins == 0, 1.0, 2.0) / N
    back_z = ahead_z.T * weight[:, None]
    ahead_y = np.concatenate([cos, sin], axis=1)
    back_y = np.concatenate([cos, -sin], axis=1) / N
    plane = ((lane % 4) * 2 + lane // 64) * 16 + (lane // 4) % 16
    cx, sx = cos[plane, :], sin[plane, :]
    ahead_x = np.block([[cx, -sx], [sx, cx]])
    back_x = np.block([[cx.T, sx.T], [-sx.T, cx.T]]) / N
    out = []
    high, low = np_split(ahead_z)
    zero = np.zeros_like(low)
    out.append(np.block([[high, low], [high, zero]]))
    high, low = np_split(back_z)
    out.append(np.block([[high, low], [high, zero]]))
    for table in (ahead_y, back_y):
        high, low = np_split(table)
        out.append(np.concatenate([high, low], axis=0))
    for table in (ahead_x, back_x):
        out.extend(np_split(table))
    return np.stack(out)


def split(value):
    high = value.astype(BF16)
    low = (value - high.astype(F32)).astype(BF16)
    return high, low


def dot(a, b):
    return lax.dot_general(a, b, (((1,), (0,)), ((), ())), preferred_element_type=F32)


def exchange_bits(first, second, shift, lane_bit):
    new_first = jnp.where(lane_bit, pltpu.roll(second, shift, 1), first)
    new_second = jnp.where(lane_bit, second, pltpu.roll(first, N - shift, 1))
    return new_first, new_second


def butterfly(tiles, lane):
    step = SLOTS // 2
    while step >= 1:
        bit = (lane & (step * 4)) != 0
        for index in range(SLOTS):
            if index & step == 0:
                tiles[index], tiles[index + step] = exchange_bits(
                    tiles[index], tiles[index + step], step * 4, bit
                )
        step //= 2
    return tiles


def turned(value, lane):
    return jnp.where((lane & 2) == 0, pltpu.roll(value, N - 2, 1), -pltpu.roll(value, 2, 1))


def z_matmul(rows, table):
    high, low = split(rows)
    both = dot(jnp.concatenate([high, low], axis=1), table)
    return both[:, :N] + both[:, N:]


def y_matmul(first, second, table, lane):
    top = jnp.concatenate([first, second], axis=1)
    low_half = jnp.concatenate([turned(first, lane), turned(second, lane)], axis=1)
    high, low = split(jnp.concatenate([top, low_half], axis=0))
    both = dot(table, high)
    return both[:N] + both[N:] + dot(table[:N], low)


def x_matmul(rows, table_high, table_low):
    count = rows.shape[0]
    high, low = split(rows)
    both = dot(jnp.concatenate([high, low], axis=0), table_high)
    return both[:count] + both[count:] + dot(high, table_low)


def stress_terms(strain, freq_x, freq_y, freq_z):
    xx, yy, zz, yz, xz, xy = strain
    trace = xx + yy + zz
    tau_xx = lame_lambda * trace + 2.0 * shear_modulus * xx
    tau_yy = lame_lambda * trace + 2.0 * shear_modulus * yy
    tau_zz = lame_lambda * trace + 2.0 * shear_modulus * zz
    tau_yz = 2.0 * shear_modulus * yz
    tau_xz = 2.0 * shear_modulus * xz
    tau_xy = 2.0 * shear_modulus * xy
    norm_x = tau_xx * freq_x + tau_xy * freq_y + tau_xz * freq_z
    norm_y = tau_xy * freq_x + tau_yy * freq_y + tau_yz * freq_z
    norm_z = tau_xz * freq_x + tau_yz * freq_y + tau_zz * freq_z
    square = freq_x * freq_x + freq_y * freq_y + freq_z * freq_z
    inverse = 1.0 / jnp.maximum(square, 1.0)
    along = (freq_x * norm_x + freq_y * norm_y + freq_z * norm_z) * inverse * inverse * green_coef
    half = inverse / (2.0 * shear_modulus)

    def term(first_q, second_q, first_n, second_n, plastic):
        total = (first_q * second_n + second_q * first_n) * half - first_q * second_q * along
        return total - plastic

    el_xx = term(freq_x, freq_x, norm_x, norm_x, xx)
    el_yy = term(freq_y, freq_y, norm_y, norm_y, yy)
    el_zz = term(freq_z, freq_z, norm_z, norm_z, zz)
    el_yz = term(freq_y, freq_z, norm_y, norm_z, yz)
    el_xz = term(freq_x, freq_z, norm_x, norm_z, xz)
    el_xy = term(freq_x, freq_y, norm_x, norm_y, xy)
    el_trace = el_xx + el_yy + el_zz
    return (
        lame_lambda * el_trace + 2.0 * shear_modulus * el_xx,
        lame_lambda * el_trace + 2.0 * shear_modulus * el_yy,
        lame_lambda * el_trace + 2.0 * shear_modulus * el_zz,
        2.0 * shear_modulus * el_yz,
        2.0 * shear_modulus * el_xz,
        2.0 * shear_modulus * el_xy,
    )


def signed_frequency(index):
    value = jnp.where(index < N // 2, index, jnp.where(index == N // 2, 0, index - N))
    return value.astype(F32)


def kernel(
    plastic_ref, table_hbm, offsets_ref, lines_ref, burgers_ref, counts_ref, voxels_ref,
    stress_ref, moved_ref,
    plastic_buf, table_buf, out1, in1, out2, in2, spec, out3, in3, out4, in4, stress_buf,
    seg, samp, lbuf, mbuf, pair_out,
    load_sem, send1, recv1, send2, recv2, send3, recv3, send4, recv4,
    halo_send, halo_recv, samp_send, samp_recv, store_sem,
):
    gx = lax.axis_index("gx")
    pa = lax.axis_index("pa")
    quarter = gx // 2
    x_low = gx % 2
    slot = x_low * 16 + pa
    left = {"gx": (gx + 7) % 8}
    right = {"gx": (gx + 1) % 8}
    cross = {"gx": (gx + 8 + 2 * x_low - 1) % 8}

    loads = [
        pltpu.make_async_copy(plastic_ref.at[pl.ds(2 * j, 2)], plastic_buf.at[pl.ds(2 * j, 2)], load_sem.at[j])
        for j in range(CHUNKS)
    ]
    table_loads = [
        pltpu.make_async_copy(table_hbm.at[i], table_buf.at[i], load_sem.at[CHUNKS + i]) for i in range(8)
    ]
    loads[0].start()
    table_loads[0].start()
    loads[1].start()
    loads[2].start()
    for i in (2, 4, 5, 6, 7, 3, 1):
        table_loads[i].start()

    def group_device(other):
        return {"gx": 2 * quarter + other // 16, "pa": other % 16}

    barrier = pltpu.get_barrier_semaphore()

    def greet(i, carry):
        pl.semaphore_signal(barrier, inc=1, device_id=group_device((slot + i) % SLOTS), device_id_type=MESH)
        return carry

    lax.fori_loop(1, SLOTS, greet, 0)
    for i in range(1, 4):
        pl.semaphore_signal(barrier, inc=1, device_id={"gx": (gx + 2 * i) % 8}, device_id_type=MESH)
    pl.semaphore_signal(barrier, inc=1, device_id=cross, device_id_type=MESH)

    lane8 = lax.broadcasted_iota(jnp.int32, (8, N), 1)
    lane32 = lax.broadcasted_iota(jnp.int32, (32, N), 1)
    lane128 = lax.broadcasted_iota(jnp.int32, (N, N), 1)

    def group_send(j, source, target, send_sem, recv_sem):
        def one(i, carry):
            other = (slot + i) % SLOTS
            pltpu.make_async_remote_copy(
                src_ref=source.at[j, other], dst_ref=target.at[j, slot],
                send_sem=send_sem.at[j], recv_sem=recv_sem.at[j],
                device_id=group_device(other), device_id_type=MESH,
            ).start()
            return carry

        lax.fori_loop(1, SLOTS, one, 0)
        pltpu.make_async_copy(source.at[j, slot], target.at[j, slot], recv_sem.at[j]).start()

    for j in range(CHUNKS):
        if j == 0:
            table_loads[0].wait()
        loads[j].wait()
        rows = plastic_buf[2 * j : 2 * j + 2].reshape(256, N)
        result = z_matmul(rows, table_buf[0])
        tiles = butterfly([result[8 * t : 8 * t + 8] for t in range(SLOTS)], lane8)
        for t in range(SLOTS):
            out1[j, t] = tiles[t]
        if j == 0:
            pl.semaphore_wait(barrier, 35)
        group_send(j, out1, in1, send1, recv1)

    counts = counts_ref[...]
    index = lax.broadcasted_iota(jnp.int32, (CELLS, N), 1)
    live = (index < counts.reshape(CELLS, 1)).astype(F32)
    first_position = []
    for k in range(3):
        value = offsets_ref[k, 0] - 0.5
        seg[HALO : HALO + CELLS, k, :] = value
        seg[HALO : HALO + CELLS, 3 + k, :] = lines_ref[k, 0]
        seg[HALO : HALO + CELLS, 6 + k, :] = burgers_ref[k, 0] * live
    to_left = pltpu.make_async_remote_copy(
        src_ref=seg.at[pl.ds(HALO, HALO)], dst_ref=seg.at[pl.ds(HALO + CELLS, HALO)],
        send_sem=halo_send.at[0], recv_sem=halo_recv.at[0], device_id=left, device_id_type=MESH,
    )
    to_right = pltpu.make_async_remote_copy(
        src_ref=seg.at[pl.ds(CELLS, HALO)], dst_ref=seg.at[pl.ds(0, HALO)],
        send_sem=halo_send.at[1], recv_sem=halo_recv.at[1], device_id=right, device_id_type=MESH,
    )
    to_left.start()
    to_right.start()

    to_left.wait()
    to_right.wait()
    line = [seg[:, 3 + k, :] for k in range(3)]
    burg = [seg[:, 6 + k, :] for k in range(3)]
    start = [seg[:, k, :] for k in range(3)]
    lbuf[...] = jnp.zeros_like(lbuf)
    mbuf[...] = jnp.zeros_like(mbuf)
    for c in range(3):
        for b in range(3):
            lbuf[:, 3 * c + b, :] = line[c] * burg[b]

    def pair_field(position, low, high):
        arm = [
            position[1] * line[2] - position[2] * line[1],
            position[2] * line[0] - position[0] * line[2],
            position[0] * line[1] - position[1] * line[0],
        ]
        for shift in range(3):
            moved_arm = [
                arm[0],
                arm[1] - (shift - 1.0) * line[2],
                arm[2] + (shift - 1.0) * line[1],
            ]
            for a in range(3):
                for b in range(3):
                    mbuf[shift, :, 3 * a + b, :] = moved_arm[a] * burg[b]
        pad = jnp.zeros((16 - WIDE, N), F32)
        columns = [jnp.transpose(jnp.concatenate([value, pad], axis=0)) for value in position]
        for cell in range(low, high):
            target = [value[cell : cell + 1] for value in position]
            weights, factors = [], []
            for shift in range(3):
                source = cell + shift - 1
                delta = [
                    target[k] - (shift - 1.0) * (k == 0) - columns[k][:, source : source + 1] for k in range(3)
                ]
                radius = delta[0] * delta[0] + delta[1] * delta[1] + delta[2] * delta[2] + core_square
                root = lax.rsqrt(radius)
                weights.append(root * root * root)
                factors.append(jnp.concatenate([lbuf[source], mbuf[shift, source]], axis=0))
            weight_high, weight_low = split(jnp.concatenate(weights, axis=0))
            factor_high, factor_low = split(jnp.concatenate(factors, axis=1))
            both = dot(jnp.concatenate([factor_high, factor_low], axis=0), weight_high)
            pair_out[cell] = both[:32] + both[32:] + dot(factor_high, weight_low)
        spread = [[pair_out[:, 3 * c + b, :] for b in range(3)] for c in range(3)]
        offset = [[pair_out[:, 16 + 3 * a + b, :] for b in range(3)] for a in range(3)]
        moment = [[None] * 3 for _ in range(3)]
        for b in range(3):
            for a in range(3):
                n, m = (a + 1) % 3, (a + 2) % 3
                moment[a][b] = position[n] * spread[m][b] - position[m] * spread[n][b] - offset[a][b]
        return [
            pair_factor * (moment[a][b] + moment[b][a])
            for a, b in ((0, 0), (1, 1), (2, 2), (1, 2), (0, 2), (0, 1))
        ]

    pair_out[...] = jnp.zeros_like(pair_out)
    field = pair_field(start, 1, WIDE - 1)

    for j in range(CHUNKS):
        pltpu.make_async_copy(in1.at[j], in1.at[j], recv1.at[j]).wait()
        if j == 0:
            table_loads[2].wait()
        result = y_matmul(
            in1[j, 0:16].reshape(N, N), in1[j, 16:32].reshape(N, N), table_buf[2], lane128
        )
        for low in range(2):
            out2[j, :, low] = result[:, N * low : N * low + N].reshape(4, 32, N)
        for i in range(1, 4):
            other = (quarter + i) % 4
            pltpu.make_async_remote_copy(
                src_ref=out2.at[j, other], dst_ref=in2.at[j, quarter],
                send_sem=send2.at[j], recv_sem=recv2.at[j],
                device_id={"gx": 2 * other + x_low}, device_id_type=MESH,
            ).start()
        pltpu.make_async_copy(out2.at[j, quarter], in2.at[j, quarter], recv2.at[j]).start()

    high_bit = (lane32 & 64) != 0
    part_bit = (lane32 & 2) != 0
    bin_bit = (lane32 & 1) != 0
    for j in range(CHUNKS):
        pltpu.make_async_copy(in2.at[j], in2.at[j], recv2.at[j]).wait()
        if j == 0:
            table_loads[4].wait()
            table_loads[5].wait()
        grid = [[in2[j, q, low] for low in range(2)] for q in range(4)]
        for q in range(4):
            grid[q][0], grid[q][1] = exchange_bits(grid[q][0], grid[q][1], 64, high_bit)
        for c in range(2):
            for q in range(2):
                grid[q][c], grid[q + 2][c] = exchange_bits(grid[q][c], grid[q + 2][c], 2, part_bit)
            for q in (0, 2):
                grid[q][c], grid[q + 1][c] = exchange_bits(grid[q][c], grid[q + 1][c], 1, bin_bit)
        rows = jnp.concatenate(
            [
                jnp.concatenate([grid[b][c], grid[2 + b][c]], axis=1)
                for c in range(2)
                for b in range(2)
            ],
            axis=0,
        )
        spec[2 * j : 2 * j + 2] = x_matmul(rows, table_buf[4], table_buf[5]).reshape(2, 2, 32, 2 * N)

    k_index = lax.broadcasted_iota(jnp.int32, (8, 2 * N), 1) % N
    freq_x = signed_frequency(k_index)
    for b in range(2):
        freq_z = (2 * slot + b).astype(F32)
        for t in range(4):
            row = lax.broadcasted_iota(jnp.int32, (8, 2 * N), 0) + 32 * quarter + 8 * t
            freq_y = signed_frequency(row)
            strain = [spec[c, b, 8 * t : 8 * t + 8, :] for c in range(6)]
            result = stress_terms(strain, freq_x, freq_y, freq_z)
            for c in range(6):
                spec[c, b, 8 * t : 8 * t + 8, :] = result[c]

    for j in range(CHUNKS):
        if j == 0:
            table_loads[6].wait()
            table_loads[7].wait()
        result = x_matmul(spec[2 * j : 2 * j + 2].reshape(N, 2 * N), table_buf[6], table_buf[7])
        grid = [[None, None] for _ in range(4)]
        for c in range(2):
            for b in range(2):
                at = 32 * (2 * c + b)
                grid[b][c] = result[at : at + 32, :N]
                grid[2 + b][c] = result[at : at + 32, N:]
        for c in range(2):
            for q in range(2):
                grid[q][c], grid[q + 2][c] = exchange_bits(grid[q][c], grid[q + 2][c], 2, part_bit)
            for q in (0, 2):
                grid[q][c], grid[q + 1][c] = exchange_bits(grid[q][c], grid[q + 1][c], 1, bin_bit)
        for q in range(4):
            grid[q][0], grid[q][1] = exchange_bits(grid[q][0], grid[q][1], 64, high_bit)
            for low in range(2):
                out3[j, q, low] = grid[q][low]
        for i in range(1, 4):
            other = (quarter + i) % 4
            pltpu.make_async_remote_copy(
                src_ref=out3.at[j, other], dst_ref=in3.at[j, quarter],
                send_sem=send3.at[j], recv_sem=recv3.at[j],
                device_id={"gx": 2 * other + x_low}, device_id_type=MESH,
            ).start()
        pltpu.make_async_copy(out3.at[j, quarter], in3.at[j, quarter], recv3.at[j]).start()

    for j in range(CHUNKS):
        pltpu.make_async_copy(in3.at[j], in3.at[j], recv3.at[j]).wait()
        if j == 0:
            table_loads[3].wait()
        result = y_matmul(
            in3[j, :, 0].reshape(N, N), in3[j, :, 1].reshape(N, N), table_buf[3], lane128
        )
        for low in range(2):
            out4[j, 16 * low : 16 * low + 16] = result[:, N * low : N * low + N].reshape(16, 8, N)
        group_send(j, out4, in4, send4, recv4)

    voxels = voxels_ref[0]
    row_of = (voxels >> 7) & 31
    z_of = voxels & 127
    sublane = lax.broadcasted_iota(jnp.int32, (8, N), 0)
    stores = []
    for j in range(CHUNKS):
        pltpu.make_async_copy(in4.at[j], in4.at[j], recv4.at[j]).wait()
        if j == 0:
            table_loads[1].wait()
        tiles = butterfly([in4[j, t] for t in range(SLOTS)], lane8)
        result = z_matmul(jnp.concatenate(tiles, axis=0), table_buf[1])
        stress_buf[2 * j : 2 * j + 2] = result.reshape(2, 16, 8, N)
        store = pltpu.make_async_copy(
            stress_buf.at[pl.ds(2 * j, 2)], stress_ref.at[pl.ds(2 * j, 2)], store_sem.at[j]
        )
        store.start()
        stores.append(store)
        for cell in range(CELLS):
            pick_z = jnp.broadcast_to(z_of[cell : cell + 1], (8, N))
            pick_row = jnp.broadcast_to(row_of[cell : cell + 1], (8, N))
            for c in range(2):
                total = jnp.zeros((8, N), F32)
                for t in range(4):
                    at = 128 * c + 32 * cell + 8 * t
                    tile = jnp.take_along_axis(result[at : at + 8], pick_z, axis=1, mode="promise_in_bounds")
                    total = total + jnp.where(pick_row == sublane + 8 * t, tile, 0.0)
                samp[HALO + cell, 2 * j + c : 2 * j + c + 1, :] = jnp.sum(total, axis=0, keepdims=True)

    samp_left = pltpu.make_async_remote_copy(
        src_ref=samp.at[pl.ds(HALO, 2)], dst_ref=samp.at[pl.ds(HALO + CELLS, 2)],
        send_sem=samp_send.at[0], recv_sem=samp_recv.at[0], device_id=left, device_id_type=MESH,
    )
    samp_right = pltpu.make_async_remote_copy(
        src_ref=samp.at[pl.ds(HALO + 2, 2)], dst_ref=samp.at[pl.ds(1, 2)],
        send_sem=samp_send.at[1], recv_sem=samp_recv.at[1], device_id=right, device_id_type=MESH,
    )
    samp_left.start()
    samp_right.start()
    samp_left.wait()
    samp_right.wait()

    sampled = [samp[:, c, :] for c in range(6)]

    def step(position, field):
        sigma = [sampled[c] + field[c] for c in range(6)]
        pull = [
            sum(sigma[full_index[a][b]] * burg[b] for b in range(3))
            for a in range(3)
        ]
        force = [
            pull[1] * line[2] - pull[2] * line[1],
            pull[2] * line[0] - pull[0] * line[2],
            pull[0] * line[1] - pull[1] * line[0],
        ]
        return [position[k] + step_size * force[k] for k in range(3)]

    position = step(start, field)
    for repeat in range(1, 3):
        field = pair_field(position, 1 + repeat, WIDE - 1 - repeat)
        position = step(position, field)
    for k in range(3):
        moved_ref[k, 0] = position[k][HALO : HALO + CELLS] - start[k][HALO : HALO + CELLS]

    for j in range(CHUNKS):
        pltpu.make_async_copy(out1.at[j, pl.ds(0, 31)], in1.at[j, pl.ds(0, 31)], send1.at[j]).wait()
        pltpu.make_async_copy(out2.at[j, pl.ds(0, 3)], in2.at[j, pl.ds(0, 3)], send2.at[j]).wait()
        pltpu.make_async_copy(out3.at[j, pl.ds(0, 3)], in3.at[j, pl.ds(0, 3)], send3.at[j]).wait()
        pltpu.make_async_copy(out4.at[j, pl.ds(0, 31)], in4.at[j, pl.ds(0, 31)], send4.at[j]).wait()
    for store in stores:
        store.wait()


def body(plastic, offsets, lines, burgers, counts, voxels):
    any_space = pl.BlockSpec(memory_space=pl.ANY)
    vmem = pl.BlockSpec(memory_space=pltpu.VMEM)
    dma = pltpu.SemaphoreType.DMA
    group = pltpu.VMEM((CHUNKS, SLOTS, 8, N), F32)
    along = pltpu.VMEM((CHUNKS, 4, 2, 32, N), F32)
    return pl.pallas_call(
        kernel,
        out_shape=(
            jax.ShapeDtypeStruct((6, 16, 8, N), F32),
            jax.ShapeDtypeStruct((3, 1, CELLS, N), F32),
        ),
        in_specs=[any_space, any_space, vmem, vmem, vmem, vmem, vmem],
        out_specs=(any_space, vmem),
        scratch_shapes=[
            pltpu.VMEM((6, 16, 8, N), F32),
            pltpu.VMEM((8, 2 * N, 2 * N), BF16),
            group, group, along, along,
            pltpu.VMEM((6, 2, 32, 2 * N), F32),
            along, along, group, group,
            pltpu.VMEM((6, 16, 8, N), F32),
            pltpu.VMEM((WIDE, 16, N), F32),
            pltpu.VMEM((WIDE, 8, N), F32),
            pltpu.VMEM((WIDE, 16, N), F32),
            pltpu.VMEM((3, WIDE, 16, N), F32),
            pltpu.VMEM((WIDE, 32, N), F32),
            dma((CHUNKS + 8,)),
            dma((CHUNKS,)), dma((CHUNKS,)), dma((CHUNKS,)), dma((CHUNKS,)),
            dma((CHUNKS,)), dma((CHUNKS,)), dma((CHUNKS,)), dma((CHUNKS,)),
            dma((2,)), dma((2,)), dma((2,)), dma((2,)), dma((CHUNKS,)),
        ],
        compiler_params=pltpu.CompilerParams(collective_id=0, has_side_effects=True),
    )(plastic, jnp.asarray(tables()), offsets, lines, burgers, counts, voxels)


def solution(mesh):
    placed = (
        P(None, "gx", "pa", None),
        P(None, "pa", "gx", None),
        P(None, "pa", "gx", None),
        P(None, "pa", "gx", None),
        P("pa", "gx"),
        P("pa", "gx", None),
    )
    return jax.shard_map(
        body,
        mesh=mesh,
        in_specs=placed,
        out_specs=(P(None, "gx", "pa", None), P(None, "pa", "gx", None)),
        check_vma=False,
    )
```

```python
import math

import jax
import jax.numpy as jnp
import numpy as np
from jax import lax
from jax.experimental import pallas as pl
from jax.experimental.pallas import tpu as pltpu
from jax.sharding import PartitionSpec as P

MESH = pl.DeviceIdType.MESH
F32 = jnp.float32
BF16 = jnp.bfloat16
N = 128
GX = 8
PA = 16
CHUNKS = ((0, 1, 2, 5, 3, 4),)
PAIRS = ((0, 1), (2, 5), (3, 4))
CELLS = 4
HALO = 3
WIDE = CELLS + 2 * HALO

lame_lambda = 1.5
shear_modulus = 1.0
green_coef = 2.5 / 3.5
core_square = 0.09
pair_factor = 1.0 / (4.0 * math.pi)
step_size = 0.05
full_index = ((0, 5, 4), (5, 1, 3), (4, 3, 2))


def np_split(table):
    table = np.asarray(table, np.float32)
    high = table.astype(jnp.bfloat16)
    low = (table - high.astype(np.float32)).astype(jnp.bfloat16)
    return high, low


def tables():
    index = np.arange(N)
    angle = 2.0 * np.pi * (np.outer(index, index) % N) / N
    cos, sin = np.cos(angle), np.sin(angle)
    flip = np.where(index % 2 == 0, 1.0, -1.0)
    bins, parity = index // 2, index % 2
    weight = np.where(bins == 0, 1.0, 2.0)[:, None] / N
    ahead_z = []
    for odd in range(2):
        imaginary = (parity == 1 - odd)[:, None]
        table = np.where(imaginary, -sin[bins], cos[bins])
        ahead_z.append(np.where(imaginary & (bins == 0)[:, None], flip[None, :], table))
    back_z = [table * weight for table in ahead_z]
    ky = np.arange(N // 2)
    ahead_y = np.concatenate([cos[:, ky], -sin[:, ky]], axis=1)
    ahead_y[:, N // 2] = flip
    back_y = ahead_y.T * np.where(index % 64 == 0, 1.0, 2.0)[:, None] / N
    plane = (index % 8) * 16 + index // 8
    cx, sx = cos[:, plane], sin[:, plane]
    ahead_x = [np.concatenate([cx, sx], axis=1), np.concatenate([sx, -cx], axis=1)]
    back_x = [np.concatenate([cx.T, -sx.T], axis=1) / N, np.concatenate([sx.T, cx.T], axis=1) / N]

    def beside(table):
        high, low = np_split(table)
        return np.block([[high, high], [low, np.zeros_like(low)]])

    def under(table):
        high, low = np_split(table)
        return np.block([[high, low], [high, np.zeros_like(low)]])

    def stacked(table):
        return np.concatenate(np_split(table), axis=0)

    out = [beside(ahead_z[0]), beside(ahead_z[1]), under(ahead_y)]
    out += [stacked(ahead_x[0]), stacked(ahead_x[1]), stacked(back_x[0]), stacked(back_x[1])]
    out += [under(back_y), beside(back_z[0].T), beside(back_z[1].T)]
    return np.stack(out), np.stack(back_z).astype(np.float32)


def split(value):
    high = value.astype(BF16)
    low = (value - high.astype(F32)).astype(BF16)
    return high, low


def dot(a, b, contract=(1, 0)):
    return lax.dot_general(a, b, (((contract[0],), (contract[1],)), ((), ())), preferred_element_type=F32)


def butterfly(value, lane):
    tiles = [value[8 * t : 8 * t + 8] for t in range(PA)]
    step = PA // 2
    while step >= 1:
        bit = (lane & (step * 8)) != 0
        for index in range(PA):
            if index & step == 0:
                first, second = tiles[index], tiles[index + step]
                tiles[index] = jnp.where(bit, pltpu.roll(second, step * 8, 1), first)
                tiles[index + step] = jnp.where(bit, second, pltpu.roll(first, N - step * 8, 1))
        step //= 2
    return jnp.concatenate(tiles, axis=0)


def turned(value, upper):
    other = pltpu.roll(value, N // 2, 1)
    return jnp.where(upper, -other, other)


def y_matmul(rows, table):
    high, low = split(rows)
    both = dot(jnp.concatenate([high, low], axis=1), table)
    return both[:, :N] + both[:, N:]


def x_matmul(table, first, second, upper):
    top = jnp.concatenate([first, second], axis=1)
    below = jnp.concatenate([turned(first, upper), turned(second, upper)], axis=1)
    high, low = split(jnp.concatenate([top, below], axis=0))
    both = dot(table, high)
    result = both[:N] + both[N:] + dot(table[:N], low)
    return result[:, :N], result[:, N:]


def stress_terms(strain, freq_x, freq_y, freq_z):
    xx, yy, zz, yz, xz, xy = strain
    trace = xx + yy + zz
    tau_xx = lame_lambda * trace + 2.0 * shear_modulus * xx
    tau_yy = lame_lambda * trace + 2.0 * shear_modulus * yy
    tau_zz = lame_lambda * trace + 2.0 * shear_modulus * zz
    tau_yz = 2.0 * shear_modulus * yz
    tau_xz = 2.0 * shear_modulus * xz
    tau_xy = 2.0 * shear_modulus * xy
    norm_x = tau_xx * freq_x + tau_xy * freq_y + tau_xz * freq_z
    norm_y = tau_xy * freq_x + tau_yy * freq_y + tau_yz * freq_z
    norm_z = tau_xz * freq_x + tau_yz * freq_y + tau_zz * freq_z
    square = freq_x * freq_x + freq_y * freq_y + freq_z * freq_z
    inverse = 1.0 / jnp.maximum(square, 1.0)
    along = (freq_x * norm_x + freq_y * norm_y + freq_z * norm_z) * inverse * inverse * green_coef
    half = inverse / (2.0 * shear_modulus)

    def term(first_q, second_q, first_n, second_n, plastic):
        total = (first_q * second_n + second_q * first_n) * half - first_q * second_q * along
        return total - plastic

    el_xx = term(freq_x, freq_x, norm_x, norm_x, xx)
    el_yy = term(freq_y, freq_y, norm_y, norm_y, yy)
    el_zz = term(freq_z, freq_z, norm_z, norm_z, zz)
    el_yz = term(freq_y, freq_z, norm_y, norm_z, yz)
    el_xz = term(freq_x, freq_z, norm_x, norm_z, xz)
    el_xy = term(freq_x, freq_y, norm_x, norm_y, xy)
    el_trace = el_xx + el_yy + el_zz
    return (
        lame_lambda * el_trace + 2.0 * shear_modulus * el_xx,
        lame_lambda * el_trace + 2.0 * shear_modulus * el_yy,
        lame_lambda * el_trace + 2.0 * shear_modulus * el_zz,
        2.0 * shear_modulus * el_yz,
        2.0 * shear_modulus * el_xz,
        2.0 * shear_modulus * el_xy,
    )


def signed_frequency(index):
    value = jnp.where(index < N // 2, index, jnp.where(index == N // 2, 0, index - N))
    return value.astype(F32)


def kernel(
    plastic_hbm, table_hbm, back_hbm, offsets_hbm, lines_hbm, burgers_hbm, counts_hbm, voxels_hbm,
    stress_hbm, moved_hbm,
    plastic_buf, table_buf, back_buf, offsets_ref, lines_ref, burgers_ref, counts_ref, voxels_ref, moved_ref,
    out1, in1, out2, in2, spec, stress_buf, seg, samp, lbuf, mbuf, pair_out,
    load_sem, send1, recv1, send2, recv2, halo_send, halo_recv, samp_send, samp_recv, store_sem,
):
    gx = lax.axis_index("gx")
    pa = lax.axis_index("pa")
    mode = pa * GX + gx
    left = {"gx": (gx + 7) % 8}
    right = {"gx": (gx + 1) % 8}
    place = {c: (j, row) for j, chunk in enumerate(CHUNKS) for row, c in enumerate(chunk)}

    def device(i):
        return {"gx": gx ^ (i & 7), "pa": pa ^ (i >> 3)}

    sources = (plastic_hbm, offsets_hbm, lines_hbm, burgers_hbm, counts_hbm, voxels_hbm, back_hbm)
    targets = (plastic_buf, offsets_ref, lines_ref, burgers_ref, counts_ref, voxels_ref, back_buf)
    loads = [
        pltpu.make_async_copy(source, target, load_sem.at[i])
        for i, (source, target) in enumerate(zip(sources, targets))
    ]
    table_loads = [
        pltpu.make_async_copy(table_hbm.at[i], table_buf.at[i], load_sem.at[len(loads) + i]) for i in range(10)
    ]
    barrier = pltpu.get_barrier_semaphore()
    with jax.named_scope("greet"):
        loads[0].start()
        table_loads[0].start()
        table_loads[1].start()
        for i in range(N - 1, 0, -1):
            pl.semaphore_signal(barrier, inc=1, device_id=device(i), device_id_type=MESH)
        for copy in loads[1:] + table_loads[2:]:
            copy.start()

    lane8 = lax.broadcasted_iota(jnp.int32, (8, N), 1)
    upper = lax.broadcasted_iota(jnp.int32, (N, N), 1) >= N // 2

    def send_all(j, source, target, send_sem, recv_sem):
        rows = pl.ds(0, len(CHUNKS[j]))
        for i in range(N - 1, 0, -1):
            pltpu.make_async_remote_copy(
                src_ref=source.at[j, mode ^ i, rows], dst_ref=target.at[j, mode, rows],
                send_sem=send_sem.at[j], recv_sem=recv_sem.at[j],
                device_id=device(i), device_id_type=MESH,
            ).start()
        pltpu.make_async_copy(source.at[j, mode, rows], target.at[j, mode, rows], recv_sem.at[j]).start()

    def wait_all(j, target, recv_sem):
        whole = target.at[j, :, pl.ds(0, len(CHUNKS[j]))]
        pltpu.make_async_copy(whole, whole, recv_sem.at[j]).wait()

    def put(target, c, value):
        j, row = place[c]
        target.reshape(len(CHUNKS) * N * 8, N)[pl.ds(j * N * 8 + row, N, stride=8), :] = value

    def take(source, c):
        j, row = place[c]
        return source.reshape(len(CHUNKS) * N * 8, N)[pl.ds(j * N * 8 + row, N, stride=8), :]

    with jax.named_scope("wait_load"):
        loads[0].wait()
        table_loads[0].wait()
        table_loads[1].wait()
    with jax.named_scope("z_ahead"):
        for pair in PAIRS:
            rows = jnp.concatenate([plastic_buf[c].reshape(N, N) for c in pair], axis=0)
            high, low = split(rows)
            both = dot(table_buf[1 if pair[0] == 3 else 0], jnp.concatenate([high, low], axis=1), (1, 1))
            result = both[:N] + both[N:]
            put(out1, pair[0], result[:, :N])
            put(out1, pair[1], result[:, N:])
    with jax.named_scope("wait_barrier"):
        pl.semaphore_wait(barrier, N - 1)
    with jax.named_scope("send1"):
        for j in range(len(CHUNKS)):
            send_all(j, out1, in1, send1, recv1)

    for copy in loads[1:6]:
        copy.wait()
    counts = counts_ref[...]
    index = lax.broadcasted_iota(jnp.int32, (CELLS, N), 1)
    live = (index < counts.reshape(CELLS, 1)).astype(F32)
    first_position = []
    for k in range(3):
        value = offsets_ref[k, 0] - 0.5
        seg[HALO : HALO + CELLS, k, :] = value
        seg[HALO : HALO + CELLS, 3 + k, :] = lines_ref[k, 0]
        seg[HALO : HALO + CELLS, 6 + k, :] = burgers_ref[k, 0] * live
    to_left = pltpu.make_async_remote_copy(
        src_ref=seg.at[pl.ds(HALO, HALO)], dst_ref=seg.at[pl.ds(HALO + CELLS, HALO)],
        send_sem=halo_send.at[0], recv_sem=halo_recv.at[0], device_id=left, device_id_type=MESH,
    )
    to_right = pltpu.make_async_remote_copy(
        src_ref=seg.at[pl.ds(CELLS, HALO)], dst_ref=seg.at[pl.ds(0, HALO)],
        send_sem=halo_send.at[1], recv_sem=halo_recv.at[1], device_id=right, device_id_type=MESH,
    )
    to_left.start()
    to_right.start()

    for copy in table_loads[2:]:
        copy.wait()
    loads[6].wait()
    for j in range(len(CHUNKS)):
        with jax.named_scope("wait_in1"):
            wait_all(j, in1, recv1)
        with jax.named_scope("y_ahead"):
            for c in CHUNKS[j]:
                spec[c] = y_matmul(butterfly(take(in1, c), lane8), table_buf[2])
    with jax.named_scope("x_ahead"):
        for pair in PAIRS:
            table = table_buf[4 if pair[0] == 3 else 3]
            spec[pair[0]], spec[pair[1]] = x_matmul(table, spec[pair[0]], spec[pair[1]], upper)

    with jax.named_scope("operator"):
        freq_y = signed_frequency(lane8 % 64)
        freq_z = jnp.where(mode % 2 == 0, mode // 2, -(mode // 2)).astype(F32)
        for t in range(N // 8):
            freq_x = signed_frequency(lax.broadcasted_iota(jnp.int32, (8, N), 0) + 8 * t)
            strain = [spec[c, 8 * t : 8 * t + 8, :] for c in range(6)]
            result = stress_terms(strain, freq_x, freq_y, freq_z)
            for c in range(6):
                spec[c, 8 * t : 8 * t + 8, :] = result[c]

    with jax.named_scope("x_back"):
        for pair in PAIRS:
            table = table_buf[6 if pair[0] == 3 else 5]
            spec[pair[0]], spec[pair[1]] = x_matmul(table, spec[pair[0]], spec[pair[1]], upper)
    for j in range(len(CHUNKS)):
        with jax.named_scope("y_back"):
            for c in CHUNKS[j]:
                put(out2, c, butterfly(y_matmul(spec[c], table_buf[7]), lane8))
        with jax.named_scope("send2"):
            send_all(j, out2, in2, send2, recv2)

    with jax.named_scope("wait_halo"):
        to_left.wait()
        to_right.wait()
    line = [seg[:, 3 + k, :] for k in range(3)]
    burg = [seg[:, 6 + k, :] for k in range(3)]
    start = [seg[:, k, :] for k in range(3)]
    lbuf[...] = jnp.zeros_like(lbuf)
    mbuf[...] = jnp.zeros_like(mbuf)
    for c in range(3):
        for b in range(3):
            lbuf[:, 3 * c + b, :] = line[c] * burg[b]

    def pair_field(position, low, high):
        arm = [
            position[1] * line[2] - position[2] * line[1],
            position[2] * line[0] - position[0] * line[2],
            position[0] * line[1] - position[1] * line[0],
        ]
        for shift in range(3):
            moved_arm = [
                arm[0],
                arm[1] - (shift - 1.0) * line[2],
                arm[2] + (shift - 1.0) * line[1],
            ]
            for a in range(3):
                for b in range(3):
                    mbuf[shift, :, 3 * a + b, :] = moved_arm[a] * burg[b]
        pad = jnp.zeros((16 - WIDE, N), F32)
        columns = [jnp.transpose(jnp.concatenate([value, pad], axis=0)) for value in position]
        for cell in range(low, high):
            target = [value[cell : cell + 1] for value in position]
            weights, factors = [], []
            for shift in range(3):
                source = cell + shift - 1
                delta = [
                    target[k] - (shift - 1.0) * (k == 0) - columns[k][:, source : source + 1] for k in range(3)
                ]
                radius = delta[0] * delta[0] + delta[1] * delta[1] + delta[2] * delta[2] + core_square
                root = lax.rsqrt(radius)
                weights.append(root * root * root)
                factors.append(jnp.concatenate([lbuf[source], mbuf[shift, source]], axis=0))
            weight_high, weight_low = split(jnp.concatenate(weights, axis=0))
            factor_high, factor_low = split(jnp.concatenate(factors, axis=1))
            both = dot(jnp.concatenate([factor_high, factor_low], axis=0), weight_high)
            pair_out[cell] = both[:32] + both[32:] + dot(factor_high, weight_low)
        spread = [[pair_out[:, 3 * c + b, :] for b in range(3)] for c in range(3)]
        offset = [[pair_out[:, 16 + 3 * a + b, :] for b in range(3)] for a in range(3)]
        moment = [[None] * 3 for _ in range(3)]
        for b in range(3):
            for a in range(3):
                n, m = (a + 1) % 3, (a + 2) % 3
                moment[a][b] = position[n] * spread[m][b] - position[m] * spread[n][b] - offset[a][b]
        return [
            pair_factor * (moment[a][b] + moment[b][a])
            for a, b in ((0, 0), (1, 1), (2, 2), (1, 2), (0, 2), (0, 1))
        ]

    pair_out[...] = jnp.zeros_like(pair_out)
    with jax.named_scope("pair1"):
        field = pair_field(start, 1, WIDE - 1)

    voxels = voxels_ref[0]
    column_of = voxels >> 7
    z_of = voxels & 127
    for j in range(len(CHUNKS)):
        with jax.named_scope("wait_in2"):
            wait_all(j, in2, recv2)
    with jax.named_scope("sample"):
        for c in range(6):
            stress_buf[c] = take(in2, c)
        for cell in range(CELLS):
            pick_z = jnp.broadcast_to(z_of[cell : cell + 1], (8, N))
            pick = jnp.broadcast_to(column_of[cell : cell + 1], (8, N))
            total = [None] * 6
            for t in range(N // 8):
                rows = slice(8 * t, 8 * t + 8)
                factor = [
                    jnp.take_along_axis(back_buf[odd, rows], pick_z, axis=1, mode="promise_in_bounds")
                    for odd in range(2)
                ]
                for c in range(6):
                    tile = jnp.take_along_axis(stress_buf[c, rows], pick, axis=1, mode="promise_in_bounds")
                    term = tile * factor[1 if c in (3, 4) else 0]
                    total[c] = term if t == 0 else total[c] + term
            for c in range(6):
                samp[HALO + cell, c : c + 1, :] = jnp.sum(total[c], axis=0, keepdims=True)

    samp_left = pltpu.make_async_remote_copy(
        src_ref=samp.at[pl.ds(HALO, 2)], dst_ref=samp.at[pl.ds(HALO + CELLS, 2)],
        send_sem=samp_send.at[0], recv_sem=samp_recv.at[0], device_id=left, device_id_type=MESH,
    )
    samp_right = pltpu.make_async_remote_copy(
        src_ref=samp.at[pl.ds(HALO + 2, 2)], dst_ref=samp.at[pl.ds(1, 2)],
        send_sem=samp_send.at[1], recv_sem=samp_recv.at[1], device_id=right, device_id_type=MESH,
    )
    samp_left.start()
    samp_right.start()
    stores = []
    with jax.named_scope("z_back"):
        for pair in PAIRS:
            table = table_buf[9 if pair[0] == 3 else 8]
            high, low = split(jnp.concatenate([stress_buf[c] for c in pair], axis=1))
            both = dot(table, jnp.concatenate([high, low], axis=0))
            result = both[:N] + both[N:]
            for c, half in zip(pair, (result[:, :N], result[:, N:])):
                plastic_buf[c] = jnp.transpose(half).reshape(16, 8, N)
                store = pltpu.make_async_copy(plastic_buf.at[c], stress_hbm.at[c], store_sem.at[c])
                store.start()
                stores.append(store)
    with jax.named_scope("wait_samp"):
        samp_left.wait()
        samp_right.wait()

    sampled = [samp[:, c, :] for c in range(6)]

    def step(position, field):
        sigma = [sampled[c] + field[c] for c in range(6)]
        pull = [
            sum(sigma[full_index[a][b]] * burg[b] for b in range(3))
            for a in range(3)
        ]
        force = [
            pull[1] * line[2] - pull[2] * line[1],
            pull[2] * line[0] - pull[0] * line[2],
            pull[0] * line[1] - pull[1] * line[0],
        ]
        return [position[k] + step_size * force[k] for k in range(3)]

    position = step(start, field)
    for repeat in range(1, 3):
        with jax.named_scope("pair_later"):
            field = pair_field(position, 1 + repeat, WIDE - 1 - repeat)
        position = step(position, field)
    for k in range(3):
        moved_ref[k, 0] = position[k][HALO : HALO + CELLS] - start[k][HALO : HALO + CELLS]
    moved_store = pltpu.make_async_copy(moved_ref, moved_hbm, store_sem.at[6])
    moved_store.start()
    stores.append(moved_store)

    with jax.named_scope("drain_mark"):
        stores[0].wait()
    for j in range(len(CHUNKS)):
        for source, send_sem in ((out1, send1), (out2, send2)):
            sent = source.at[j, pl.ds(0, N - 1), pl.ds(0, len(CHUNKS[j]))]
            pltpu.make_async_copy(sent, sent, send_sem.at[j]).wait()
    for store in stores[1:]:
        store.wait()


def body(plastic, offsets, lines, burgers, counts, voxels):
    any_space = pl.BlockSpec(memory_space=pl.ANY)
    dma = pltpu.SemaphoreType.DMA
    group = pltpu.VMEM((len(CHUNKS), N, 8, N), F32)
    vectors = pltpu.VMEM((3, 1, CELLS, N), F32)
    table, back = tables()
    return pl.pallas_call(
        kernel,
        out_shape=(
            jax.ShapeDtypeStruct((6, 16, 8, N), F32),
            jax.ShapeDtypeStruct((3, 1, CELLS, N), F32),
        ),
        in_specs=[any_space] * 8,
        out_specs=(any_space, any_space),
        scratch_shapes=[
            pltpu.VMEM((6, 16, 8, N), F32),
            pltpu.VMEM((10, 2 * N, 2 * N), BF16),
            pltpu.VMEM((2, N, N), F32),
            vectors, vectors, vectors,
            pltpu.VMEM((1, CELLS), jnp.int32),
            pltpu.VMEM((1, CELLS, N), jnp.int32),
            vectors,
            group, group, group, group,
            pltpu.VMEM((6, N, N), F32),
            pltpu.VMEM((6, N, N), F32),
            pltpu.VMEM((WIDE, 16, N), F32),
            pltpu.VMEM((WIDE, 8, N), F32),
            pltpu.VMEM((WIDE, 16, N), F32),
            pltpu.VMEM((3, WIDE, 16, N), F32),
            pltpu.VMEM((WIDE, 32, N), F32),
            dma((17,)),
            dma((len(CHUNKS),)), dma((len(CHUNKS),)), dma((len(CHUNKS),)), dma((len(CHUNKS),)),
            dma((2,)), dma((2,)), dma((2,)), dma((2,)), dma((7,)),
        ],
        compiler_params=pltpu.CompilerParams(collective_id=0, has_side_effects=True),
    )(plastic, jnp.asarray(table), jnp.asarray(back), offsets, lines, burgers, counts, voxels)


def solution(mesh):
    placed = (
        P(None, "gx", "pa", None),
        P(None, "pa", "gx", None),
        P(None, "pa", "gx", None),
        P(None, "pa", "gx", None),
        P("pa", "gx"),
        P("pa", "gx", None),
    )
    return jax.shard_map(
        body,
        mesh=mesh,
        in_specs=placed,
        out_specs=(P(None, "gx", "pa", None), P(None, "pa", "gx", None)),
        check_vma=False,
    )
```

```python
import math

import jax
import jax.numpy as jnp
import numpy as np
from jax import lax
from jax.experimental import pallas as pl
from jax.experimental.pallas import tpu as pltpu
from jax.sharding import PartitionSpec as P

MESH = pl.DeviceIdType.MESH
F32 = jnp.float32
BF16 = jnp.bfloat16
N = 128
GX = 8
PA = 16
CHUNKS = ((0, 1, 2, 5, 3, 4),)
PAIRS = ((0, 1), (2, 5), (3, 4))
CELLS = 4
HALO = 3
WIDE = CELLS + 2 * HALO
OWN_SECOND = ((3, (1, 2), True), (4, (0, 1, 2), True), (5, (0, 1, 2), True), (6, (0, 1), True))
REST_SECOND = ((2, (0, 1, 2), True), (3, (0,), False), (6, (2,), False), (7, (0, 1, 2), True))
OWN_THIRD = ((4, (1, 2), True), (5, (0, 1), True))
REST_THIRD = ((3, (0, 1, 2), True), (4, (0,), False), (5, (2,), False), (6, (0, 1, 2), True))

lame_lambda = 1.5
shear_modulus = 1.0
green_coef = 2.5 / 3.5
core_square = 0.09
pair_factor = 1.0 / (4.0 * math.pi)
step_size = 0.05
full_index = ((0, 5, 4), (5, 1, 3), (4, 3, 2))


def np_split(table):
    table = np.asarray(table, np.float32)
    high = table.astype(jnp.bfloat16)
    low = (table - high.astype(np.float32)).astype(jnp.bfloat16)
    return high, low


def tables():
    index = np.arange(N)
    angle = 2.0 * np.pi * (np.outer(index, index) % N) / N
    cos, sin = np.cos(angle), np.sin(angle)
    flip = np.where(index % 2 == 0, 1.0, -1.0)
    bins, parity = index // 2, index % 2
    weight = np.where(bins == 0, 1.0, 2.0)[:, None] / N
    ahead_z = []
    for odd in range(2):
        imaginary = (parity == 1 - odd)[:, None]
        table = np.where(imaginary, -sin[bins], cos[bins])
        ahead_z.append(np.where(imaginary & (bins == 0)[:, None], flip[None, :], table))
    back_z = [table * weight for table in ahead_z]
    ky = np.arange(N // 2)
    ahead_y = np.concatenate([cos[:, ky], -sin[:, ky]], axis=1)
    ahead_y[:, N // 2] = flip
    back_y = ahead_y.T * np.where(index % 64 == 0, 1.0, 2.0)[:, None] / N
    plane = (index % 8) * 16 + index // 8
    cx, sx = cos[:, plane], sin[:, plane]
    ahead_x = [np.concatenate([cx, sx], axis=1), np.concatenate([sx, -cx], axis=1)]
    back_x = [np.concatenate([cx.T, -sx.T], axis=1) / N, np.concatenate([sx.T, cx.T], axis=1) / N]

    def beside(table):
        high, low = np_split(table)
        return np.block([[high, high], [low, np.zeros_like(low)]])

    def under(table):
        high, low = np_split(table)
        return np.block([[high, low], [high, np.zeros_like(low)]])

    def stacked(table):
        return np.concatenate(np_split(table), axis=0)

    out = [beside(ahead_z[0]), beside(ahead_z[1]), under(ahead_y)]
    out += [stacked(ahead_x[0]), stacked(ahead_x[1]), stacked(back_x[0]), stacked(back_x[1])]
    out += [under(back_y), beside(back_z[0].T), beside(back_z[1].T)]
    return np.stack(out), np.stack(back_z).astype(np.float32)


def split(value):
    high = value.astype(BF16)
    low = (value - high.astype(F32)).astype(BF16)
    return high, low


def dot(a, b, contract=(1, 0)):
    return lax.dot_general(a, b, (((contract[0],), (contract[1],)), ((), ())), preferred_element_type=F32)


def butterfly(value, lane):
    tiles = [value[8 * t : 8 * t + 8] for t in range(PA)]
    step = PA // 2
    while step >= 1:
        bit = (lane & (step * 8)) != 0
        for index in range(PA):
            if index & step == 0:
                first, second = tiles[index], tiles[index + step]
                tiles[index] = jnp.where(bit, pltpu.roll(second, step * 8, 1), first)
                tiles[index + step] = jnp.where(bit, second, pltpu.roll(first, N - step * 8, 1))
        step //= 2
    return jnp.concatenate(tiles, axis=0)


def turned(value, upper):
    other = pltpu.roll(value, N // 2, 1)
    return jnp.where(upper, -other, other)


def y_matmul(rows, table):
    high, low = split(rows)
    both = dot(jnp.concatenate([high, low], axis=1), table)
    return both[:, :N] + both[:, N:]


def x_matmul(table, first, second, upper):
    top = jnp.concatenate([first, second], axis=1)
    below = jnp.concatenate([turned(first, upper), turned(second, upper)], axis=1)
    high, low = split(jnp.concatenate([top, below], axis=0))
    both = dot(table, high)
    result = both[:N] + both[N:] + dot(table[:N], low)
    return result[:, :N], result[:, N:]


def stress_terms(strain, freq_x, freq_y, freq_z):
    xx, yy, zz, yz, xz, xy = strain
    trace = xx + yy + zz
    tau_xx = lame_lambda * trace + 2.0 * shear_modulus * xx
    tau_yy = lame_lambda * trace + 2.0 * shear_modulus * yy
    tau_zz = lame_lambda * trace + 2.0 * shear_modulus * zz
    tau_yz = 2.0 * shear_modulus * yz
    tau_xz = 2.0 * shear_modulus * xz
    tau_xy = 2.0 * shear_modulus * xy
    norm_x = tau_xx * freq_x + tau_xy * freq_y + tau_xz * freq_z
    norm_y = tau_xy * freq_x + tau_yy * freq_y + tau_yz * freq_z
    norm_z = tau_xz * freq_x + tau_yz * freq_y + tau_zz * freq_z
    square = freq_x * freq_x + freq_y * freq_y + freq_z * freq_z
    inverse = 1.0 / jnp.maximum(square, 1.0)
    along = (freq_x * norm_x + freq_y * norm_y + freq_z * norm_z) * inverse * inverse * green_coef
    half = inverse / (2.0 * shear_modulus)

    def term(first_q, second_q, first_n, second_n, plastic):
        total = (first_q * second_n + second_q * first_n) * half - first_q * second_q * along
        return total - plastic

    el_xx = term(freq_x, freq_x, norm_x, norm_x, xx)
    el_yy = term(freq_y, freq_y, norm_y, norm_y, yy)
    el_zz = term(freq_z, freq_z, norm_z, norm_z, zz)
    el_yz = term(freq_y, freq_z, norm_y, norm_z, yz)
    el_xz = term(freq_x, freq_z, norm_x, norm_z, xz)
    el_xy = term(freq_x, freq_y, norm_x, norm_y, xy)
    el_trace = el_xx + el_yy + el_zz
    return (
        lame_lambda * el_trace + 2.0 * shear_modulus * el_xx,
        lame_lambda * el_trace + 2.0 * shear_modulus * el_yy,
        lame_lambda * el_trace + 2.0 * shear_modulus * el_zz,
        2.0 * shear_modulus * el_yz,
        2.0 * shear_modulus * el_xz,
        2.0 * shear_modulus * el_xy,
    )


def partners():
    hops = (0, 1, 2, 1)

    def distance(i):
        low, high = i & 7, i >> 3
        return hops[2 * (high >> 3) + (low & 1)] + hops[low >> 1] + hops[(high >> 1) & 3]

    return sorted(range(1, N), key=lambda i: -distance(i))


def signed_frequency(index):
    value = jnp.where(index < N // 2, index, jnp.where(index == N // 2, 0, index - N))
    return value.astype(F32)


def arms_into(mbuf, position, line, burg):
    arm = [
        position[1] * line[2] - position[2] * line[1],
        position[2] * line[0] - position[0] * line[2],
        position[0] * line[1] - position[1] * line[0],
    ]
    for shift in range(3):
        moved_arm = [
            arm[0],
            arm[1] - (shift - 1.0) * line[2],
            arm[2] + (shift - 1.0) * line[1],
        ]
        for a in range(3):
            for b in range(3):
                mbuf[shift, :, 3 * a + b, :] = moved_arm[a] * burg[b]


def pair_blocks(position, lbuf, mbuf, pair_out, blocks):
    pad = jnp.zeros((16 - WIDE, N), F32)
    columns = [jnp.transpose(jnp.concatenate([value, pad], axis=0)) for value in position]
    for cell, shifts, fresh in blocks:
        target = [value[cell : cell + 1] for value in position]
        weights, factors = [], []
        for shift in shifts:
            source = cell + shift - 1
            delta = [
                (target[k] - (shift - 1.0) * (k == 0)) - columns[k][:, source : source + 1] for k in range(3)
            ]
            radius = delta[0] * delta[0] + delta[1] * delta[1] + delta[2] * delta[2] + core_square
            root = lax.rsqrt(radius)
            weights.append(root * root * root)
            factors.append(jnp.concatenate([lbuf[source], mbuf[shift, source]], axis=0))
        weight_high, weight_low = split(jnp.concatenate(weights, axis=0))
        factor_high, factor_low = split(jnp.concatenate(factors, axis=1))
        both = dot(jnp.concatenate([factor_high, factor_low], axis=0), weight_high)
        total = both[:32] + both[32:] + dot(factor_high, weight_low)
        pair_out[cell] = total if fresh else pair_out[cell] + total


def pair_field(position, pair_out):
    spread = [[pair_out[:, 3 * c + b, :] for b in range(3)] for c in range(3)]
    offset = [[pair_out[:, 16 + 3 * a + b, :] for b in range(3)] for a in range(3)]
    moment = [[None] * 3 for _ in range(3)]
    for b in range(3):
        for a in range(3):
            n, m = (a + 1) % 3, (a + 2) % 3
            moment[a][b] = position[n] * spread[m][b] - position[m] * spread[n][b] - offset[a][b]
    return [
        pair_factor * (moment[a][b] + moment[b][a])
        for a, b in ((0, 0), (1, 1), (2, 2), (1, 2), (0, 2), (0, 1))
    ]


def advance(position, sampled, field, line, burg):
    sigma = [sampled[c] + field[c] for c in range(6)]
    pull = [sum(sigma[full_index[a][b]] * burg[b] for b in range(3)) for a in range(3)]
    force = [
        pull[1] * line[2] - pull[2] * line[1],
        pull[2] * line[0] - pull[0] * line[2],
        pull[0] * line[1] - pull[1] * line[0],
    ]
    return [position[k] + step_size * force[k] for k in range(3)]


def kernel(
    plastic_hbm, table_hbm, back_hbm, offsets_hbm, lines_hbm, burgers_hbm, counts_hbm, voxels_hbm,
    stress_out, seg_out, samp_out, field_out, lbuf, second_out, third_out,
    plastic_buf, table_buf, back_buf, offsets_ref, lines_ref, burgers_ref, counts_ref, voxels_ref,
    out1, in1, out2, in2, spec, stress_buf, seg, samp, own, mbuf, pair_out, factor_buf,
    load_sem, send1, recv1, send2, recv2, halo_send, halo_recv, samp_send, samp_recv,
):
    gx = lax.axis_index("gx")
    pa = lax.axis_index("pa")
    mode = pa * GX + gx
    left = {"gx": (gx + 7) % 8}
    right = {"gx": (gx + 1) % 8}
    place = {c: (j, row) for j, chunk in enumerate(CHUNKS) for row, c in enumerate(chunk)}

    def device(i):
        return {"gx": gx ^ (i & 7), "pa": pa ^ (i >> 3)}

    sources = (plastic_hbm, offsets_hbm, lines_hbm, burgers_hbm, counts_hbm, voxels_hbm, back_hbm)
    targets = (plastic_buf, offsets_ref, lines_ref, burgers_ref, counts_ref, voxels_ref, back_buf)
    loads = [
        pltpu.make_async_copy(source, target, load_sem.at[i])
        for i, (source, target) in enumerate(zip(sources, targets))
    ]
    table_loads = [
        pltpu.make_async_copy(table_hbm.at[i], table_buf.at[i], load_sem.at[len(loads) + i]) for i in range(10)
    ]
    barrier = pltpu.get_barrier_semaphore()
    with jax.named_scope("greet"):
        loads[0].start()
        table_loads[0].start()
        table_loads[1].start()
        for i in partners():
            pl.semaphore_signal(barrier, inc=1, device_id=device(i), device_id_type=MESH)
        for copy in loads[1:] + table_loads[2:]:
            copy.start()

    lane8 = lax.broadcasted_iota(jnp.int32, (8, N), 1)
    upper = lax.broadcasted_iota(jnp.int32, (N, N), 1) >= N // 2

    def send_all(j, source, target, send_sem, recv_sem):
        rows = pl.ds(0, len(CHUNKS[j]))
        for i in partners():
            pltpu.make_async_remote_copy(
                src_ref=source.at[j, mode ^ i, rows], dst_ref=target.at[j, mode, rows],
                send_sem=send_sem.at[j], recv_sem=recv_sem.at[j],
                device_id=device(i), device_id_type=MESH,
            ).start()
        pltpu.make_async_copy(source.at[j, mode, rows], target.at[j, mode, rows], recv_sem.at[j]).start()

    def wait_all(j, target, recv_sem):
        whole = target.at[j, :, pl.ds(0, len(CHUNKS[j]))]
        pltpu.make_async_copy(whole, whole, recv_sem.at[j]).wait()

    def put(target, c, value):
        j, row = place[c]
        target.reshape(len(CHUNKS) * N * 8, N)[pl.ds(j * N * 8 + row, N, stride=8), :] = value

    def take(source, c):
        j, row = place[c]
        return source.reshape(len(CHUNKS) * N * 8, N)[pl.ds(j * N * 8 + row, N, stride=8), :]

    with jax.named_scope("wait_load"):
        loads[0].wait()
        table_loads[0].wait()
        table_loads[1].wait()
    with jax.named_scope("z_ahead"):
        for pair in PAIRS:
            rows = jnp.concatenate([plastic_buf[c].reshape(N, N) for c in pair], axis=0)
            high, low = split(rows)
            both = dot(table_buf[1 if pair[0] == 3 else 0], jnp.concatenate([high, low], axis=1), (1, 1))
            result = both[:N] + both[N:]
            put(out1, pair[0], result[:, :N])
            put(out1, pair[1], result[:, N:])
    with jax.named_scope("wait_barrier"):
        pl.semaphore_wait(barrier, N - 1)
    with jax.named_scope("send1"):
        for j in range(len(CHUNKS)):
            send_all(j, out1, in1, send1, recv1)

    for copy in loads[1:6]:
        copy.wait()
    counts = counts_ref[...]
    index = lax.broadcasted_iota(jnp.int32, (CELLS, N), 1)
    live = (index < counts.reshape(CELLS, 1)).astype(F32)
    first_position = []
    for k in range(3):
        value = offsets_ref[k, 0] - 0.5
        seg[HALO : HALO + CELLS, k, :] = value
        seg[HALO : HALO + CELLS, 3 + k, :] = lines_ref[k, 0]
        seg[HALO : HALO + CELLS, 6 + k, :] = burgers_ref[k, 0] * live
    to_left = pltpu.make_async_remote_copy(
        src_ref=seg.at[pl.ds(HALO, HALO)], dst_ref=seg.at[pl.ds(HALO + CELLS, HALO)],
        send_sem=halo_send.at[0], recv_sem=halo_recv.at[0], device_id=left, device_id_type=MESH,
    )
    to_right = pltpu.make_async_remote_copy(
        src_ref=seg.at[pl.ds(CELLS, HALO)], dst_ref=seg.at[pl.ds(0, HALO)],
        send_sem=halo_send.at[1], recv_sem=halo_recv.at[1], device_id=right, device_id_type=MESH,
    )
    to_left.start()
    to_right.start()

    for copy in table_loads[2:]:
        copy.wait()
    loads[6].wait()
    for j in range(len(CHUNKS)):
        with jax.named_scope("wait_in1"):
            wait_all(j, in1, recv1)
        with jax.named_scope("y_ahead"):
            for c in CHUNKS[j]:
                spec[c] = y_matmul(butterfly(take(in1, c), lane8), table_buf[2])
    with jax.named_scope("x_ahead"):
        for pair in PAIRS:
            table = table_buf[4 if pair[0] == 3 else 3]
            spec[pair[0]], spec[pair[1]] = x_matmul(table, spec[pair[0]], spec[pair[1]], upper)

    with jax.named_scope("operator"):
        freq_y = signed_frequency(lane8 % 64)
        freq_z = jnp.where(mode % 2 == 0, mode // 2, -(mode // 2)).astype(F32)
        for t in range(N // 8):
            freq_x = signed_frequency(lax.broadcasted_iota(jnp.int32, (8, N), 0) + 8 * t)
            strain = [spec[c, 8 * t : 8 * t + 8, :] for c in range(6)]
            result = stress_terms(strain, freq_x, freq_y, freq_z)
            for c in range(6):
                spec[c, 8 * t : 8 * t + 8, :] = result[c]

    with jax.named_scope("x_back"):
        for pair in PAIRS:
            table = table_buf[6 if pair[0] == 3 else 5]
            spec[pair[0]], spec[pair[1]] = x_matmul(table, spec[pair[0]], spec[pair[1]], upper)
    for j in range(len(CHUNKS)):
        with jax.named_scope("y_back"):
            for c in CHUNKS[j]:
                put(out2, c, butterfly(y_matmul(spec[c], table_buf[7]), lane8))
        with jax.named_scope("send2"):
            send_all(j, out2, in2, send2, recv2)

    with jax.named_scope("wait_halo"):
        to_left.wait()
        to_right.wait()
    line = [seg[:, 3 + k, :] for k in range(3)]
    burg = [seg[:, 6 + k, :] for k in range(3)]
    start = [seg[:, k, :] for k in range(3)]
    seg_out[...] = seg[...]
    with jax.named_scope("pair1"):
        lbuf[...] = jnp.zeros_like(lbuf)
        mbuf[...] = jnp.zeros_like(mbuf)
        pair_out[...] = jnp.zeros_like(pair_out)
        own[...] = jnp.zeros_like(own)
        for c in range(3):
            for b in range(3):
                lbuf[:, 3 * c + b, :] = line[c] * burg[b]
        arms_into(mbuf, start, line, burg)
        pair_blocks(start, lbuf, mbuf, pair_out, [(cell, (0, 1, 2), True) for cell in range(1, WIDE - 1)])
        field = pair_field(start, pair_out)
        for c in range(6):
            field_out[c] = field[c]
        second_out[...] = jnp.zeros_like(second_out)
        third_out[...] = jnp.zeros_like(third_out)

    voxels = voxels_ref[0]
    column_of = voxels >> 7
    z_of = voxels & 127
    with jax.named_scope("factors"):
        for cell in range(CELLS):
            pick_z = jnp.broadcast_to(z_of[cell : cell + 1], (8, N))
            for odd in range(2):
                for t in range(N // 8):
                    rows = slice(8 * t, 8 * t + 8)
                    factor_buf[cell, odd, rows] = jnp.take_along_axis(
                        back_buf[odd, rows], pick_z, axis=1, mode="promise_in_bounds"
                    )
    for j in range(len(CHUNKS)):
        with jax.named_scope("wait_in2"):
            wait_all(j, in2, recv2)
    with jax.named_scope("sample"):
        for c in range(6):
            stress_buf[c] = take(in2, c)
        for cell in range(CELLS):
            pick = jnp.broadcast_to(column_of[cell : cell + 1], (8, N))
            total = [None] * 6
            for t in range(N // 8):
                rows = slice(8 * t, 8 * t + 8)
                factor = [factor_buf[cell, odd, rows] for odd in range(2)]
                for c in range(6):
                    tile = jnp.take_along_axis(stress_buf[c, rows], pick, axis=1, mode="promise_in_bounds")
                    term = tile * factor[1 if c in (3, 4) else 0]
                    total[c] = term if t == 0 else total[c] + term
            for c in range(6):
                value = jnp.sum(total[c], axis=0, keepdims=True)
                samp[HALO + cell, c : c + 1, :] = value
                own[HALO + cell, c : c + 1, :] = value

    samp_left = pltpu.make_async_remote_copy(
        src_ref=samp.at[pl.ds(HALO, 2)], dst_ref=samp.at[pl.ds(HALO + CELLS, 2)],
        send_sem=samp_send.at[0], recv_sem=samp_recv.at[0], device_id=left, device_id_type=MESH,
    )
    samp_right = pltpu.make_async_remote_copy(
        src_ref=samp.at[pl.ds(HALO + 2, 2)], dst_ref=samp.at[pl.ds(1, 2)],
        send_sem=samp_send.at[1], recv_sem=samp_recv.at[1], device_id=right, device_id_type=MESH,
    )
    samp_left.start()
    samp_right.start()
    with jax.named_scope("z_back"):
        for pair in PAIRS:
            table = table_buf[9 if pair[0] == 3 else 8]
            high, low = split(jnp.concatenate([stress_buf[c] for c in pair], axis=1))
            both = dot(table, jnp.concatenate([high, low], axis=0))
            result = both[:N] + both[N:]
            for c, half in zip(pair, (result[:, :N], result[:, N:])):
                stress_out[c] = jnp.transpose(half).reshape(16, 8, N)
    with jax.named_scope("pair_own"):
        position = advance(start, [own[:, c, :] for c in range(6)], field, line, burg)
        arms_into(mbuf, position, line, burg)
        pair_blocks(position, lbuf, mbuf, second_out, OWN_SECOND)
        position = advance(
            position, [own[:, c, :] for c in range(6)], pair_field(position, second_out), line, burg
        )
        arms_into(mbuf, position, line, burg)
        pair_blocks(position, lbuf, mbuf, third_out, OWN_THIRD)

    with jax.named_scope("wait_samp"):
        samp_left.wait()
        samp_right.wait()
    for c in range(6):
        samp_out[c] = samp[:, c, :]

    for j in range(len(CHUNKS)):
        for source, send_sem in ((out1, send1), (out2, send2)):
            sent = source.at[j, pl.ds(0, N - 1), pl.ds(0, len(CHUNKS[j]))]
            pltpu.make_async_copy(sent, sent, send_sem.at[j]).wait()


def finish(
    stress_ref, seg, samp, field_ref, lbuf, second, third, stress_hbm, moved_hbm,
    mbuf, second_buf, third_buf, moved_ref, store_sem,
):
    store = pltpu.make_async_copy(stress_ref, stress_hbm, store_sem.at[0])
    store.start()
    line = [seg[:, 3 + k, :] for k in range(3)]
    burg = [seg[:, 6 + k, :] for k in range(3)]
    start = [seg[:, k, :] for k in range(3)]
    sampled = [samp[c] for c in range(6)]
    second_buf[...] = second[...]
    third_buf[...] = third[...]
    mbuf[...] = jnp.zeros_like(mbuf)
    with jax.named_scope("pair_second"):
        position = advance(start, sampled, [field_ref[c] for c in range(6)], line, burg)
        arms_into(mbuf, position, line, burg)
        pair_blocks(position, lbuf, mbuf, second_buf, REST_SECOND)
    with jax.named_scope("pair_third"):
        position = advance(position, sampled, pair_field(position, second_buf), line, burg)
        arms_into(mbuf, position, line, burg)
        pair_blocks(position, lbuf, mbuf, third_buf, REST_THIRD)
    with jax.named_scope("last"):
        position = advance(position, sampled, pair_field(position, third_buf), line, burg)
        for k in range(3):
            moved_ref[k, 0] = position[k][HALO : HALO + CELLS] - start[k][HALO : HALO + CELLS]
    moved_store = pltpu.make_async_copy(moved_ref, moved_hbm, store_sem.at[1])
    moved_store.start()
    store.wait()
    moved_store.wait()


def body(plastic, offsets, lines, burgers, counts, voxels):
    any_space = pl.BlockSpec(memory_space=pl.ANY)
    dma = pltpu.SemaphoreType.DMA
    group = pltpu.VMEM((len(CHUNKS), N, 8, N), F32)
    vectors = pltpu.VMEM((3, 1, CELLS, N), F32)
    table, back = tables()
    vmem = pl.BlockSpec(memory_space=pltpu.VMEM)
    state = pl.pallas_call(
        kernel,
        out_shape=(
            pltpu.VMEM((6, 16, 8, N), F32),
            pltpu.VMEM((WIDE, 16, N), F32),
            pltpu.VMEM((6, WIDE, N), F32),
            pltpu.VMEM((6, WIDE, N), F32),
            pltpu.VMEM((WIDE, 16, N), F32),
            pltpu.VMEM((WIDE, 32, N), F32),
            pltpu.VMEM((WIDE, 32, N), F32),
        ),
        in_specs=[any_space] * 8,
        out_specs=(vmem,) * 7,
        scratch_shapes=[
            pltpu.VMEM((6, 16, 8, N), F32),
            pltpu.VMEM((10, 2 * N, 2 * N), BF16),
            pltpu.VMEM((2, N, N), F32),
            vectors, vectors, vectors,
            pltpu.VMEM((1, CELLS), jnp.int32),
            pltpu.VMEM((1, CELLS, N), jnp.int32),
            group, group, group, group,
            pltpu.VMEM((6, N, N), F32),
            pltpu.VMEM((6, N, N), F32),
            pltpu.VMEM((WIDE, 16, N), F32),
            pltpu.VMEM((WIDE, 8, N), F32),
            pltpu.VMEM((WIDE, 8, N), F32),
            pltpu.VMEM((3, WIDE, 16, N), F32),
            pltpu.VMEM((WIDE, 32, N), F32),
            pltpu.VMEM((CELLS, 2, N, N), F32),
            dma((17,)),
            dma((len(CHUNKS),)), dma((len(CHUNKS),)), dma((len(CHUNKS),)), dma((len(CHUNKS),)),
            dma((2,)), dma((2,)), dma((2,)), dma((2,)),
        ],
        compiler_params=pltpu.CompilerParams(collective_id=0, has_side_effects=True),
    )(plastic, jnp.asarray(table), jnp.asarray(back), offsets, lines, burgers, counts, voxels)
    return pl.pallas_call(
        finish,
        out_shape=(
            jax.ShapeDtypeStruct((6, 16, 8, N), F32),
            jax.ShapeDtypeStruct((3, 1, CELLS, N), F32),
        ),
        in_specs=[vmem] * 7,
        out_specs=(any_space, any_space),
        scratch_shapes=[
            pltpu.VMEM((3, WIDE, 16, N), F32),
            pltpu.VMEM((WIDE, 32, N), F32),
            pltpu.VMEM((WIDE, 32, N), F32),
            vectors,
            dma((2,)),
        ],
    )(*[pltpu.with_memory_space_constraint(array, pltpu.VMEM) for array in state])


def solution(mesh):
    placed = (
        P(None, "gx", "pa", None),
        P(None, "pa", "gx", None),
        P(None, "pa", "gx", None),
        P(None, "pa", "gx", None),
        P("pa", "gx"),
        P("pa", "gx", None),
    )
    return jax.shard_map(
        body,
        mesh=mesh,
        in_specs=placed,
        out_specs=(P(None, "gx", "pa", None), P(None, "pa", "gx", None)),
        check_vma=False,
    )
```

```python
import math

import jax
import jax.numpy as jnp
import numpy as np
from jax import lax
from jax.experimental import pallas as pl
from jax.experimental.pallas import tpu as pltpu
from jax.sharding import PartitionSpec as P

MESH = pl.DeviceIdType.MESH
F32 = jnp.float32
BF16 = jnp.bfloat16
N = 128
GX = 8
PA = 16
CHUNKS = ((0, 1, 2, 5, 3, 4),)
PAIRS = ((0, 1), (2, 5), (3, 4))
CELLS = 4
HALO = 3
WIDE = CELLS + 2 * HALO
LATE = 8
OWN_SECOND = ((2, (1, 2)), (3, (0, 1, 2)), (4, (0, 1, 2)), (5, (0, 1)))
REST_SECOND = ((1, (0, 1, 2)), (2, (0,)), (5, (2,)), (6, (0, 1, 2)))
OWN_THIRD = ((3, (1, 2)), (4, (0, 1)))
REST_THIRD = ((2, (0, 1, 2)), (3, (0,)), (4, (2,)), (5, (0, 1, 2)))

lame_lambda = 1.5
shear_modulus = 1.0
green_coef = 2.5 / 3.5
core_square = 0.09
pair_factor = 1.0 / (4.0 * math.pi)
step_size = 0.05
full_index = ((0, 5, 4), (5, 1, 3), (4, 3, 2))


def np_split(table):
    table = np.asarray(table, np.float32)
    high = table.astype(jnp.bfloat16)
    low = (table - high.astype(np.float32)).astype(jnp.bfloat16)
    return high, low


def tables():
    index = np.arange(N)
    angle = 2.0 * np.pi * (np.outer(index, index) % N) / N
    cos, sin = np.cos(angle), np.sin(angle)
    flip = np.where(index % 2 == 0, 1.0, -1.0)
    bins, parity = index // 2, index % 2
    weight = np.where(bins == 0, 1.0, 2.0)[:, None] / N
    ahead_z = []
    for odd in range(2):
        imaginary = (parity == 1 - odd)[:, None]
        table = np.where(imaginary, -sin[bins], cos[bins])
        ahead_z.append(np.where(imaginary & (bins == 0)[:, None], flip[None, :], table))
    back_z = [table * weight for table in ahead_z]
    ky = np.arange(N // 2)
    ahead_y = np.concatenate([cos[:, ky], -sin[:, ky]], axis=1)
    ahead_y[:, N // 2] = flip
    back_y = ahead_y.T * np.where(index % 64 == 0, 1.0, 2.0)[:, None] / N
    plane = (index % 8) * 16 + index // 8
    cx, sx = cos[:, plane], sin[:, plane]
    ahead_x = [np.concatenate([cx, sx], axis=1), np.concatenate([sx, -cx], axis=1)]
    back_x = [np.concatenate([cx.T, -sx.T], axis=1) / N, np.concatenate([sx.T, cx.T], axis=1) / N]

    def beside(table):
        high, low = np_split(table)
        return np.block([[high, high], [low, np.zeros_like(low)]])

    def under(table):
        high, low = np_split(table)
        return np.block([[high, low], [high, np.zeros_like(low)]])

    def stacked(table):
        return np.concatenate(np_split(table), axis=0)

    out = [beside(ahead_z[0]), beside(ahead_z[1]), under(ahead_y)]
    out += [stacked(ahead_x[0]), stacked(ahead_x[1]), stacked(back_x[0]), stacked(back_x[1])]
    out += [under(back_y), beside(back_z[0].T), beside(back_z[1].T)]
    return np.stack(out), np.stack(back_z).astype(np.float32)


def split(value):
    high = value.astype(BF16)
    low = (value - high.astype(F32)).astype(BF16)
    return high, low


def dot(a, b, contract=(1, 0)):
    return lax.dot_general(a, b, (((contract[0],), (contract[1],)), ((), ())), preferred_element_type=F32)


def butterfly(value, lane):
    tiles = [value[8 * t : 8 * t + 8] for t in range(PA)]
    step = PA // 2
    while step >= 1:
        bit = (lane & (step * 8)) != 0
        for index in range(PA):
            if index & step == 0:
                first, second = tiles[index], tiles[index + step]
                going = jnp.where(bit, first, second)
                if step * 8 == N // 2:
                    gone = pltpu.roll(going, N // 2, 1)
                else:
                    gone = jnp.take_along_axis(going, lane ^ (step * 8), axis=1, mode="promise_in_bounds")
                tiles[index] = jnp.where(bit, gone, first)
                tiles[index + step] = jnp.where(bit, second, gone)
        step //= 2
    return jnp.concatenate(tiles, axis=0)


def turned(value, sign):
    return pltpu.roll(value, N // 2, 1) * sign


def y_matmul(rows, table):
    high, low = split(rows)
    both = dot(jnp.concatenate([high, low], axis=1), table)
    return both[:, :N] + both[:, N:]


def x_matmul(table, first, second, upper):
    top = jnp.concatenate([first, second], axis=1)
    below = jnp.concatenate([turned(first, upper), turned(second, upper)], axis=1)
    high, low = split(jnp.concatenate([top, below], axis=0))
    both = dot(table, high)
    result = both[:N] + both[N:] + dot(table[:N], low)
    return result[:, :N], result[:, N:]


def stress_terms(strain, freq_x, freq_y, freq_z):
    xx, yy, zz, yz, xz, xy = strain
    trace = xx + yy + zz
    tau_xx = lame_lambda * trace + 2.0 * shear_modulus * xx
    tau_yy = lame_lambda * trace + 2.0 * shear_modulus * yy
    tau_zz = lame_lambda * trace + 2.0 * shear_modulus * zz
    tau_yz = 2.0 * shear_modulus * yz
    tau_xz = 2.0 * shear_modulus * xz
    tau_xy = 2.0 * shear_modulus * xy
    norm_x = tau_xx * freq_x + tau_xy * freq_y + tau_xz * freq_z
    norm_y = tau_xy * freq_x + tau_yy * freq_y + tau_yz * freq_z
    norm_z = tau_xz * freq_x + tau_yz * freq_y + tau_zz * freq_z
    square = freq_x * freq_x + freq_y * freq_y + freq_z * freq_z
    inverse = 1.0 / jnp.maximum(square, 1.0)
    along = (freq_x * norm_x + freq_y * norm_y + freq_z * norm_z) * inverse * inverse * green_coef
    half = inverse / (2.0 * shear_modulus)

    def term(first_q, second_q, first_n, second_n, plastic):
        total = (first_q * second_n + second_q * first_n) * half - first_q * second_q * along
        return total - plastic

    el_xx = term(freq_x, freq_x, norm_x, norm_x, xx)
    el_yy = term(freq_y, freq_y, norm_y, norm_y, yy)
    el_zz = term(freq_z, freq_z, norm_z, norm_z, zz)
    el_yz = term(freq_y, freq_z, norm_y, norm_z, yz)
    el_xz = term(freq_x, freq_z, norm_x, norm_z, xz)
    el_xy = term(freq_x, freq_y, norm_x, norm_y, xy)
    el_trace = el_xx + el_yy + el_zz
    return (
        lame_lambda * el_trace + 2.0 * shear_modulus * el_xx,
        lame_lambda * el_trace + 2.0 * shear_modulus * el_yy,
        lame_lambda * el_trace + 2.0 * shear_modulus * el_zz,
        2.0 * shear_modulus * el_yz,
        2.0 * shear_modulus * el_xz,
        2.0 * shear_modulus * el_xy,
    )


def partners():
    hops = (0.0, 1.0, 2.3, 1.6)

    def distance(i):
        low, high = i & 7, i >> 3
        return hops[2 * (high >> 3) + (low & 1)] + hops[low >> 1] + hops[(high >> 1) & 3]

    return sorted(range(1, N), key=lambda i: -distance(i))


def signed_frequency(index):
    value = jnp.where(index < N // 2, index, jnp.where(index == N // 2, 0, index - N))
    return value.astype(F32)


def row_of_cells(ref, row, first, count):
    cells, rows = ref.shape[0], ref.shape[1]
    return ref.reshape(cells * rows, N)[pl.ds(first * rows + row, count, stride=rows), :]


def arms_into(mbuf, position, line, burg):
    cells = position[0].shape[0]
    flat = mbuf.reshape(3 * mbuf.shape[1] * 16, N)
    arm = [
        position[1] * line[2] - position[2] * line[1],
        position[2] * line[0] - position[0] * line[2],
        position[0] * line[1] - position[1] * line[0],
    ]
    for shift in range(3):
        moved_arm = [
            arm[0],
            arm[1] - (shift - 1.0) * line[2],
            arm[2] + (shift - 1.0) * line[1],
        ]
        for a in range(3):
            for b in range(3):
                at = shift * mbuf.shape[1] * 16 + 3 * a + b
                flat[pl.ds(at, cells, stride=16), :] = moved_arm[a] * burg[b]


def pair_blocks(position, lbuf, mbuf, pair_out, blocks, before=None):
    cells = position[0].shape[0]
    extra = (WIDE - cells) // 2
    if cells % 8:
        pad = jnp.zeros((16 - cells, N), F32)
        columns = [jnp.transpose(jnp.concatenate([value, pad], axis=0)) for value in position]
    else:
        columns = [jnp.transpose(value) for value in position]
    for cell, shifts in blocks:
        target = [value[cell : cell + 1] for value in position]
        weights, factors = [], []
        for shift in shifts:
            source = cell + shift - 1
            delta = [
                (target[k] - (shift - 1.0) * (k == 0)) - columns[k][:, source : source + 1] for k in range(3)
            ]
            radius = delta[0] * delta[0] + delta[1] * delta[1] + delta[2] * delta[2] + core_square
            root = lax.rsqrt(radius)
            weights.append(root * root * root)
            factors.append(jnp.concatenate([lbuf[source + extra], mbuf[shift, source]], axis=0))
        weight_high, weight_low = split(jnp.concatenate(weights, axis=0))
        factor_high, factor_low = split(jnp.concatenate(factors, axis=1))
        both = dot(jnp.concatenate([factor_high, factor_low], axis=0), weight_high)
        total = both[:32] + both[32:] + dot(factor_high, weight_low)
        if before is not None and len(shifts) < 3:
            total = total + before[cell]
        pair_out[cell] = total


def pair_field(position, pair_out):
    cells = position[0].shape[0]
    spread = [[row_of_cells(pair_out, 3 * c + b, 0, cells) for b in range(3)] for c in range(3)]
    offset = [[row_of_cells(pair_out, 16 + 3 * a + b, 0, cells) for b in range(3)] for a in range(3)]
    moment = [[None] * 3 for _ in range(3)]
    for b in range(3):
        for a in range(3):
            n, m = (a + 1) % 3, (a + 2) % 3
            moment[a][b] = position[n] * spread[m][b] - position[m] * spread[n][b] - offset[a][b]
    return [
        pair_factor * (moment[a][b] + moment[b][a])
        for a, b in ((0, 0), (1, 1), (2, 2), (1, 2), (0, 2), (0, 1))
    ]


def advance(position, sampled, field, line, burg):
    sigma = [sampled[c] + field[c] for c in range(6)]
    pull = [sum(sigma[full_index[a][b]] * burg[b] for b in range(3)) for a in range(3)]
    force = [
        pull[1] * line[2] - pull[2] * line[1],
        pull[2] * line[0] - pull[0] * line[2],
        pull[0] * line[1] - pull[1] * line[0],
    ]
    return [position[k] + step_size * force[k] for k in range(3)]


def kernel(
    plastic_hbm, table_hbm, back_hbm, offsets_hbm, lines_hbm, burgers_hbm, counts_hbm, voxels_hbm,
    stress_out, seg_out, samp_out, field_out, lbuf, second_out, third_out,
    plastic_buf, table_buf, back_buf, offsets_ref, lines_ref, burgers_ref, counts_ref, voxels_ref,
    out1, in1, out2, in2, spec, stress_buf, seg, samp, own, mbuf, mlate, pair_out, factor_buf,
    load_sem, send1, recv1, send2, recv2, halo_send, halo_recv, samp_send, samp_recv,
):
    gx = lax.axis_index("gx")
    pa = lax.axis_index("pa")
    mode = pa * GX + gx
    left = {"gx": (gx + 7) % 8}
    right = {"gx": (gx + 1) % 8}
    place = {c: (j, row) for j, chunk in enumerate(CHUNKS) for row, c in enumerate(chunk)}

    def device(i):
        return {"gx": gx ^ (i & 7), "pa": pa ^ (i >> 3)}

    sources = (plastic_hbm, offsets_hbm, lines_hbm, burgers_hbm, counts_hbm, voxels_hbm, back_hbm)
    targets = (plastic_buf, offsets_ref, lines_ref, burgers_ref, counts_ref, voxels_ref, back_buf)
    loads = [
        pltpu.make_async_copy(source, target, load_sem.at[i])
        for i, (source, target) in enumerate(zip(sources, targets))
    ]
    table_loads = [
        pltpu.make_async_copy(table_hbm.at[i], table_buf.at[i], load_sem.at[len(loads) + i]) for i in range(10)
    ]
    barrier = pltpu.get_barrier_semaphore()
    with jax.named_scope("greet"):
        loads[0].start()
        table_loads[0].start()
        table_loads[1].start()
        for i in partners():
            pl.semaphore_signal(barrier, inc=1, device_id=device(i), device_id_type=MESH)
        for copy in loads[1:] + table_loads[2:]:
            copy.start()

    lane8 = lax.broadcasted_iota(jnp.int32, (8, N), 1)
    upper = jnp.where(lax.broadcasted_iota(jnp.int32, (N, N), 1) >= N // 2, -1.0, 1.0)

    def send_all(j, source, target, send_sem, recv_sem):
        rows = pl.ds(0, len(CHUNKS[j]))
        for i in partners():
            pltpu.make_async_remote_copy(
                src_ref=source.at[j, mode ^ i, rows], dst_ref=target.at[j, mode, rows],
                send_sem=send_sem.at[j], recv_sem=recv_sem.at[j],
                device_id=device(i), device_id_type=MESH,
            ).start()
        pltpu.make_async_copy(source.at[j, mode, rows], target.at[j, mode, rows], recv_sem.at[j]).start()

    def wait_all(j, target, recv_sem):
        whole = target.at[j, :, pl.ds(0, len(CHUNKS[j]))]
        pltpu.make_async_copy(whole, whole, recv_sem.at[j]).wait()

    def put(target, c, value):
        j, row = place[c]
        target.reshape(len(CHUNKS) * N * 8, N)[pl.ds(j * N * 8 + row, N, stride=8), :] = value

    def take(source, c):
        j, row = place[c]
        return source.reshape(len(CHUNKS) * N * 8, N)[pl.ds(j * N * 8 + row, N, stride=8), :]

    with jax.named_scope("wait_load"):
        loads[0].wait()
        table_loads[0].wait()
        table_loads[1].wait()
    with jax.named_scope("z_ahead"):
        for pair in PAIRS:
            rows = jnp.concatenate([plastic_buf[c].reshape(N, N) for c in pair], axis=0)
            high, low = split(rows)
            both = dot(table_buf[1 if pair[0] == 3 else 0], jnp.concatenate([high, low], axis=1), (1, 1))
            result = both[:N] + both[N:]
            put(out1, pair[0], result[:, :N])
            put(out1, pair[1], result[:, N:])
    with jax.named_scope("wait_barrier"):
        pl.semaphore_wait(barrier, N - 1)
    with jax.named_scope("send1"):
        for j in range(len(CHUNKS)):
            send_all(j, out1, in1, send1, recv1)

    for copy in loads[1:6]:
        copy.wait()
    counts = counts_ref[...]
    index = lax.broadcasted_iota(jnp.int32, (CELLS, N), 1)
    live = (index < counts.reshape(CELLS, 1)).astype(F32)
    first_position = []
    for k in range(3):
        value = offsets_ref[k, 0] - 0.5
        seg[HALO : HALO + CELLS, k, :] = value
        seg[HALO : HALO + CELLS, 3 + k, :] = lines_ref[k, 0]
        seg[HALO : HALO + CELLS, 6 + k, :] = burgers_ref[k, 0] * live
    to_left = pltpu.make_async_remote_copy(
        src_ref=seg.at[pl.ds(HALO, HALO)], dst_ref=seg.at[pl.ds(HALO + CELLS, HALO)],
        send_sem=halo_send.at[0], recv_sem=halo_recv.at[0], device_id=left, device_id_type=MESH,
    )
    to_right = pltpu.make_async_remote_copy(
        src_ref=seg.at[pl.ds(CELLS, HALO)], dst_ref=seg.at[pl.ds(0, HALO)],
        send_sem=halo_send.at[1], recv_sem=halo_recv.at[1], device_id=right, device_id_type=MESH,
    )
    to_left.start()
    to_right.start()

    for copy in table_loads[2:]:
        copy.wait()
    loads[6].wait()
    for j in range(len(CHUNKS)):
        with jax.named_scope("wait_in1"):
            wait_all(j, in1, recv1)
        with jax.named_scope("y_ahead"):
            for c in CHUNKS[j]:
                spec[c] = y_matmul(butterfly(take(in1, c), lane8), table_buf[2])
    with jax.named_scope("x_ahead"):
        for pair in PAIRS:
            table = table_buf[4 if pair[0] == 3 else 3]
            spec[pair[0]], spec[pair[1]] = x_matmul(table, spec[pair[0]], spec[pair[1]], upper)

    with jax.named_scope("operator"):
        freq_y = signed_frequency(lane8 % 64)
        freq_z = jnp.where(mode % 2 == 0, mode // 2, -(mode // 2)).astype(F32)
        for t in range(N // 8):
            freq_x = signed_frequency(lax.broadcasted_iota(jnp.int32, (8, N), 0) + 8 * t)
            strain = [spec[c, 8 * t : 8 * t + 8, :] for c in range(6)]
            result = stress_terms(strain, freq_x, freq_y, freq_z)
            for c in range(6):
                spec[c, 8 * t : 8 * t + 8, :] = result[c]

    with jax.named_scope("x_back"):
        for pair in PAIRS:
            table = table_buf[6 if pair[0] == 3 else 5]
            spec[pair[0]], spec[pair[1]] = x_matmul(table, spec[pair[0]], spec[pair[1]], upper)
    for j in range(len(CHUNKS)):
        with jax.named_scope("y_back"):
            for c in CHUNKS[j]:
                put(out2, c, butterfly(y_matmul(spec[c], table_buf[7]), lane8))
        with jax.named_scope("send2"):
            send_all(j, out2, in2, send2, recv2)

    with jax.named_scope("wait_halo"):
        to_left.wait()
        to_right.wait()
    start, line, burg = ([row_of_cells(seg, 3 * i + k, 0, WIDE) for k in range(3)] for i in range(3))
    for i, part in enumerate((start, line, burg)):
        for k in range(3):
            seg_out[3 * i + k] = part[k][1 : 1 + LATE]
    with jax.named_scope("pair1"):
        lbuf[...] = jnp.zeros_like(lbuf)
        mbuf[...] = jnp.zeros_like(mbuf)
        mlate[...] = jnp.zeros_like(mlate)
        pair_out[...] = jnp.zeros_like(pair_out)
        own[...] = jnp.zeros_like(own)
        flat = lbuf.reshape(WIDE * 16, N)
        for c in range(3):
            for b in range(3):
                flat[pl.ds(3 * c + b, WIDE, stride=16), :] = line[c] * burg[b]
        arms_into(mbuf, start, line, burg)
        pair_blocks(start, lbuf, mbuf, pair_out, [(cell, (0, 1, 2)) for cell in range(1, WIDE - 1)])
        field = pair_field(start, pair_out)
        for c in range(6):
            field_out[c] = field[c][1 : 1 + LATE]
        second_out[...] = jnp.zeros_like(second_out)
        third_out[...] = jnp.zeros_like(third_out)

    voxels = voxels_ref[0]
    column_of = voxels >> 7
    z_of = voxels & 127
    with jax.named_scope("factors"):
        for cell in range(CELLS):
            pick_z = jnp.broadcast_to(z_of[cell : cell + 1], (8, N))
            for odd in range(2):
                for t in range(N // 8):
                    rows = slice(8 * t, 8 * t + 8)
                    factor_buf[cell, odd, rows] = jnp.take_along_axis(
                        back_buf[odd, rows], pick_z, axis=1, mode="promise_in_bounds"
                    )
    for j in range(len(CHUNKS)):
        with jax.named_scope("wait_in2"):
            wait_all(j, in2, recv2)
    with jax.named_scope("sample"):
        for c in range(6):
            stress_buf[c] = take(in2, c)
        for cell in range(CELLS):
            pick = jnp.broadcast_to(column_of[cell : cell + 1], (8, N))
            total = [None] * 6
            for t in range(N // 8):
                rows = slice(8 * t, 8 * t + 8)
                factor = [factor_buf[cell, odd, rows] for odd in range(2)]
                for c in range(6):
                    tile = jnp.take_along_axis(stress_buf[c, rows], pick, axis=1, mode="promise_in_bounds")
                    term = tile * factor[1 if c in (3, 4) else 0]
                    total[c] = term if t == 0 else total[c] + term
            for c in range(6):
                value = jnp.sum(total[c], axis=0, keepdims=True)
                samp[HALO + cell, c : c + 1, :] = value
                own[HALO + cell, c : c + 1, :] = value

    samp_left = pltpu.make_async_remote_copy(
        src_ref=samp.at[pl.ds(HALO, 2)], dst_ref=samp.at[pl.ds(HALO + CELLS, 2)],
        send_sem=samp_send.at[0], recv_sem=samp_recv.at[0], device_id=left, device_id_type=MESH,
    )
    samp_right = pltpu.make_async_remote_copy(
        src_ref=samp.at[pl.ds(HALO + 2, 2)], dst_ref=samp.at[pl.ds(1, 2)],
        send_sem=samp_send.at[1], recv_sem=samp_recv.at[1], device_id=right, device_id_type=MESH,
    )
    samp_left.start()
    samp_right.start()
    with jax.named_scope("z_back"):
        for pair in PAIRS:
            table = table_buf[9 if pair[0] == 3 else 8]
            high, low = split(jnp.concatenate([stress_buf[c] for c in pair], axis=1))
            both = dot(table, jnp.concatenate([high, low], axis=0))
            result = both[:N] + both[N:]
            for c, half in zip(pair, (result[:, :N], result[:, N:])):
                stress_out[c] = jnp.transpose(half).reshape(16, 8, N)
    with jax.named_scope("pair_own"):
        start, line, burg = ([seg_out[3 * i + k] for k in range(3)] for i in range(3))
        sampled = [row_of_cells(own, c, 1, LATE) for c in range(6)]
        position = advance(start, sampled, [field_out[c] for c in range(6)], line, burg)
        arms_into(mlate, position, line, burg)
        pair_blocks(position, lbuf, mlate, second_out, OWN_SECOND)
        position = advance(position, sampled, pair_field(position, second_out), line, burg)
        arms_into(mlate, position, line, burg)
        pair_blocks(position, lbuf, mlate, third_out, OWN_THIRD)

    with jax.named_scope("wait_samp"):
        samp_left.wait()
        samp_right.wait()
    for c in range(6):
        samp_out[c] = row_of_cells(samp, c, 1, LATE)

    for j in range(len(CHUNKS)):
        for source, send_sem in ((out1, send1), (out2, send2)):
            sent = source.at[j, pl.ds(0, N - 1), pl.ds(0, len(CHUNKS[j]))]
            pltpu.make_async_copy(sent, sent, send_sem.at[j]).wait()


def finish(
    stress_ref, seg, samp, field_ref, lbuf, second, third, stress_hbm, moved_hbm,
    mbuf, second_buf, third_buf, moved_ref, store_sem,
):
    store = pltpu.make_async_copy(stress_ref, stress_hbm, store_sem.at[0])
    store.start()
    start, line, burg = ([seg[3 * i + k] for k in range(3)] for i in range(3))
    sampled = [samp[c] for c in range(6)]
    for cell in (0, 3, 4, 7):
        second_buf[cell] = second[cell]
    for cell in (0, 1, 6, 7):
        third_buf[cell] = third[cell]
    with jax.named_scope("pair_second"):
        position = advance(start, sampled, [field_ref[c] for c in range(6)], line, burg)
        arms_into(mbuf, position, line, burg)
        pair_blocks(position, lbuf, mbuf, second_buf, REST_SECOND, second)
    with jax.named_scope("pair_third"):
        position = advance(position, sampled, pair_field(position, second_buf), line, burg)
        arms_into(mbuf, position, line, burg)
        pair_blocks(position, lbuf, mbuf, third_buf, REST_THIRD, third)
    with jax.named_scope("last"):
        position = advance(position, sampled, pair_field(position, third_buf), line, burg)
        for k in range(3):
            moved_ref[k, 0] = (position[k] - start[k])[2 : 2 + CELLS]
    moved_store = pltpu.make_async_copy(moved_ref, moved_hbm, store_sem.at[1])
    moved_store.start()
    store.wait()
    moved_store.wait()


def body(plastic, offsets, lines, burgers, counts, voxels):
    any_space = pl.BlockSpec(memory_space=pl.ANY)
    dma = pltpu.SemaphoreType.DMA
    group = pltpu.VMEM((len(CHUNKS), N, 8, N), F32)
    vectors = pltpu.VMEM((3, 1, CELLS, N), F32)
    table, back = tables()
    vmem = pl.BlockSpec(memory_space=pltpu.VMEM)
    state = pl.pallas_call(
        kernel,
        out_shape=(
            pltpu.VMEM((6, 16, 8, N), F32),
            pltpu.VMEM((9, LATE, N), F32),
            pltpu.VMEM((6, LATE, N), F32),
            pltpu.VMEM((6, LATE, N), F32),
            pltpu.VMEM((WIDE, 16, N), F32),
            pltpu.VMEM((LATE, 32, N), F32),
            pltpu.VMEM((LATE, 32, N), F32),
        ),
        in_specs=[any_space] * 8,
        out_specs=(vmem,) * 7,
        scratch_shapes=[
            pltpu.VMEM((6, 16, 8, N), F32),
            pltpu.VMEM((10, 2 * N, 2 * N), BF16),
            pltpu.VMEM((2, N, N), F32),
            vectors, vectors, vectors,
            pltpu.VMEM((1, CELLS), jnp.int32),
            pltpu.VMEM((1, CELLS, N), jnp.int32),
            group, group, group, group,
            pltpu.VMEM((6, N, N), F32),
            pltpu.VMEM((6, N, N), F32),
            pltpu.VMEM((WIDE, 16, N), F32),
            pltpu.VMEM((WIDE, 8, N), F32),
            pltpu.VMEM((WIDE, 8, N), F32),
            pltpu.VMEM((3, WIDE, 16, N), F32),
            pltpu.VMEM((3, LATE, 16, N), F32),
            pltpu.VMEM((WIDE, 32, N), F32),
            pltpu.VMEM((CELLS, 2, N, N), F32),
            dma((17,)),
            dma((len(CHUNKS),)), dma((len(CHUNKS),)), dma((len(CHUNKS),)), dma((len(CHUNKS),)),
            dma((2,)), dma((2,)), dma((2,)), dma((2,)),
        ],
        compiler_params=pltpu.CompilerParams(collective_id=0, has_side_effects=True),
    )(plastic, jnp.asarray(table), jnp.asarray(back), offsets, lines, burgers, counts, voxels)
    return pl.pallas_call(
        finish,
        out_shape=(
            jax.ShapeDtypeStruct((6, 16, 8, N), F32),
            jax.ShapeDtypeStruct((3, 1, CELLS, N), F32),
        ),
        in_specs=[vmem] * 7,
        out_specs=(any_space, any_space),
        scratch_shapes=[
            pltpu.VMEM((3, LATE, 16, N), F32),
            pltpu.VMEM((LATE, 32, N), F32),
            pltpu.VMEM((LATE, 32, N), F32),
            vectors,
            dma((2,)),
        ],
    )(*[pltpu.with_memory_space_constraint(array, pltpu.VMEM) for array in state])


def solution(mesh):
    placed = (
        P(None, "gx", "pa", None),
        P(None, "pa", "gx", None),
        P(None, "pa", "gx", None),
        P(None, "pa", "gx", None),
        P("pa", "gx"),
        P("pa", "gx", None),
    )
    return jax.shard_map(
        body,
        mesh=mesh,
        in_specs=placed,
        out_specs=(P(None, "gx", "pa", None), P(None, "pa", "gx", None)),
        check_vma=False,
    )
```

```python
import math

import jax
import jax.numpy as jnp
import numpy as np
from jax import lax
from jax.experimental import pallas as pl
from jax.experimental.pallas import tpu as pltpu
from jax.sharding import PartitionSpec as P

MESH = pl.DeviceIdType.MESH
F32 = jnp.float32
BF16 = jnp.bfloat16
N = 128
GX = 8
PA = 16
PAIRS = ((0, 1), (2, 5), (3, 4))
CELLS = 4
HALO = 3
WIDE = CELLS + 2 * HALO
LATE = 8
OWN_SECOND = ((2, (1, 2)), (3, (0, 1, 2)), (4, (0, 1, 2)), (5, (0, 1)))
REST_SECOND = ((1, (0, 1, 2)), (2, (0,)), (5, (2,)), (6, (0, 1, 2)))
OWN_THIRD = ((3, (1, 2)), (4, (0, 1)))
REST_THIRD = ((2, (0, 1, 2)), (3, (0,)), (4, (2,)), (5, (0, 1, 2)))

lame_lambda = 1.5
shear_modulus = 1.0
green_coef = 2.5 / 3.5
core_square = 0.09
pair_factor = 1.0 / (4.0 * math.pi)
step_size = 0.05
full_index = ((0, 5, 4), (5, 1, 3), (4, 3, 2))


def np_split(table):
    table = np.asarray(table, np.float32)
    high = table.astype(jnp.bfloat16)
    low = (table - high.astype(np.float32)).astype(jnp.bfloat16)
    return high, low


def tables():
    index = np.arange(N)
    angle = 2.0 * np.pi * (np.outer(index, index) % N) / N
    cos, sin = np.cos(angle), np.sin(angle)
    flip = np.where(index % 2 == 0, 1.0, -1.0)
    bins, parity = index // 2, index % 2
    weight = np.where(bins == 0, 1.0, 2.0)[:, None] / N
    ahead_z = []
    for odd in range(2):
        imaginary = (parity == 1 - odd)[:, None]
        table = np.where(imaginary, -sin[bins], cos[bins])
        ahead_z.append(np.where(imaginary & (bins == 0)[:, None], flip[None, :], table))
    back_z = [table * weight for table in ahead_z]
    ky = np.arange(N // 2)
    ahead_y = np.concatenate([cos[:, ky], -sin[:, ky]], axis=1)
    ahead_y[:, N // 2] = flip
    back_y = ahead_y.T * np.where(index % 64 == 0, 1.0, 2.0)[:, None] / N
    plane = (index % 8) * 16 + index // 8
    cx, sx = cos[:, plane], sin[:, plane]
    ahead_x = [np.concatenate([cx, sx], axis=1), np.concatenate([sx, -cx], axis=1)]
    back_x = [np.concatenate([cx.T, -sx.T], axis=1) / N, np.concatenate([sx.T, cx.T], axis=1) / N]

    def beside(table):
        high, low = np_split(table)
        return np.block([[high, high], [low, np.zeros_like(low)]])

    def under(table):
        high, low = np_split(table)
        return np.block([[high, low], [high, np.zeros_like(low)]])

    def stacked(table):
        return np.concatenate(np_split(table), axis=0)

    out = [beside(ahead_z[0]), beside(ahead_z[1]), under(ahead_y)]
    out += [stacked(ahead_x[0]), stacked(ahead_x[1]), stacked(back_x[0]), stacked(back_x[1])]
    out += [under(back_y), beside(back_z[0].T), beside(back_z[1].T)]
    return np.stack(out), np.stack(back_z).astype(np.float32)


def split(value):
    high = value.astype(BF16)
    low = (value - high.astype(F32)).astype(BF16)
    return high, low


def dot(a, b, contract=(1, 0)):
    return lax.dot_general(a, b, (((contract[0],), (contract[1],)), ((), ())), preferred_element_type=F32)


def butterfly(value, lane):
    tiles = [value[8 * t : 8 * t + 8] for t in range(PA)]
    step = PA // 2
    while step >= 1:
        bit = (lane & (step * 8)) != 0
        for index in range(PA):
            if index & step == 0:
                first, second = tiles[index], tiles[index + step]
                going = jnp.where(bit, first, second)
                if step * 8 == N // 2:
                    gone = pltpu.roll(going, N // 2, 1)
                else:
                    gone = jnp.take_along_axis(going, lane ^ (step * 8), axis=1, mode="promise_in_bounds")
                tiles[index] = jnp.where(bit, gone, first)
                tiles[index + step] = jnp.where(bit, second, gone)
        step //= 2
    return jnp.concatenate(tiles, axis=0)


def turned(value, sign):
    return pltpu.roll(value, N // 2, 1) * sign


def y_matmul(rows, table):
    high, low = split(rows)
    both = dot(jnp.concatenate([high, low], axis=1), table)
    return both[:, :N] + both[:, N:]


def x_matmul(table, first, second, upper):
    top = jnp.concatenate([first, second], axis=1)
    below = jnp.concatenate([turned(first, upper), turned(second, upper)], axis=1)
    high, low = split(jnp.concatenate([top, below], axis=0))
    both = dot(table, high)
    result = both[:N] + both[N:] + dot(table[:N], low)
    return result[:, :N], result[:, N:]


def stress_terms(strain, freq_x, freq_y, freq_z):
    xx, yy, zz, yz, xz, xy = strain
    trace = xx + yy + zz
    tau_xx = lame_lambda * trace + 2.0 * shear_modulus * xx
    tau_yy = lame_lambda * trace + 2.0 * shear_modulus * yy
    tau_zz = lame_lambda * trace + 2.0 * shear_modulus * zz
    tau_yz = 2.0 * shear_modulus * yz
    tau_xz = 2.0 * shear_modulus * xz
    tau_xy = 2.0 * shear_modulus * xy
    norm_x = tau_xx * freq_x + tau_xy * freq_y + tau_xz * freq_z
    norm_y = tau_xy * freq_x + tau_yy * freq_y + tau_yz * freq_z
    norm_z = tau_xz * freq_x + tau_yz * freq_y + tau_zz * freq_z
    square = freq_x * freq_x + freq_y * freq_y + freq_z * freq_z
    inverse = 1.0 / jnp.maximum(square, 1.0)
    along = (freq_x * norm_x + freq_y * norm_y + freq_z * norm_z) * inverse * inverse * green_coef
    half = inverse / (2.0 * shear_modulus)

    def term(first_q, second_q, first_n, second_n, plastic):
        total = (first_q * second_n + second_q * first_n) * half - first_q * second_q * along
        return total - plastic

    el_xx = term(freq_x, freq_x, norm_x, norm_x, xx)
    el_yy = term(freq_y, freq_y, norm_y, norm_y, yy)
    el_zz = term(freq_z, freq_z, norm_z, norm_z, zz)
    el_yz = term(freq_y, freq_z, norm_y, norm_z, yz)
    el_xz = term(freq_x, freq_z, norm_x, norm_z, xz)
    el_xy = term(freq_x, freq_y, norm_x, norm_y, xy)
    el_trace = el_xx + el_yy + el_zz
    return (
        lame_lambda * el_trace + 2.0 * shear_modulus * el_xx,
        lame_lambda * el_trace + 2.0 * shear_modulus * el_yy,
        lame_lambda * el_trace + 2.0 * shear_modulus * el_zz,
        2.0 * shear_modulus * el_yz,
        2.0 * shear_modulus * el_xz,
        2.0 * shear_modulus * el_xy,
    )


def partners():
    hops = (0.0, 1.0, 2.3, 1.6)

    def distance(i):
        low, high = i & 7, i >> 3
        return hops[2 * (high >> 3) + (low & 1)] + hops[low >> 1] + hops[(high >> 1) & 3]

    return sorted(range(1, N), key=lambda i: -distance(i))


def signed_frequency(index):
    value = jnp.where(index < N // 2, index, jnp.where(index == N // 2, 0, index - N))
    return value.astype(F32)


def row_of_cells(ref, row, first, count):
    cells, rows = ref.shape[0], ref.shape[1]
    return ref.reshape(cells * rows, N)[pl.ds(first * rows + row, count, stride=rows), :]


def arms_into(mbuf, position, line, burg):
    cells = position[0].shape[0]
    flat = mbuf.reshape(3 * mbuf.shape[1] * 16, N)
    arm = [
        position[1] * line[2] - position[2] * line[1],
        position[2] * line[0] - position[0] * line[2],
        position[0] * line[1] - position[1] * line[0],
    ]
    for shift in range(3):
        moved_arm = [
            arm[0],
            arm[1] - (shift - 1.0) * line[2],
            arm[2] + (shift - 1.0) * line[1],
        ]
        for a in range(3):
            for b in range(3):
                at = shift * mbuf.shape[1] * 16 + 3 * a + b
                flat[pl.ds(at, cells, stride=16), :] = moved_arm[a] * burg[b]


def pair_blocks(position, lbuf, mbuf, pair_out, blocks, before=None):
    cells = position[0].shape[0]
    extra = (WIDE - cells) // 2
    if cells % 8:
        pad = jnp.zeros((16 - cells, N), F32)
        columns = [jnp.transpose(jnp.concatenate([value, pad], axis=0)) for value in position]
    else:
        columns = [jnp.transpose(value) for value in position]
    for cell, shifts in blocks:
        target = [value[cell : cell + 1] for value in position]
        weights, factors = [], []
        for shift in shifts:
            source = cell + shift - 1
            delta = [
                (target[k] - (shift - 1.0) * (k == 0)) - columns[k][:, source : source + 1] for k in range(3)
            ]
            radius = delta[0] * delta[0] + delta[1] * delta[1] + delta[2] * delta[2] + core_square
            root = lax.rsqrt(radius)
            weights.append(root * root * root)
            factors.append(jnp.concatenate([lbuf[source + extra], mbuf[shift, source]], axis=0))
        weight_high, weight_low = split(jnp.concatenate(weights, axis=0))
        factor_high, factor_low = split(jnp.concatenate(factors, axis=1))
        both = dot(jnp.concatenate([factor_high, factor_low], axis=0), weight_high)
        total = both[:32] + both[32:] + dot(factor_high, weight_low)
        if before is not None and len(shifts) < 3:
            total = total + before[cell]
        pair_out[cell] = total


def pair_field(position, pair_out):
    cells = position[0].shape[0]
    spread = [[row_of_cells(pair_out, 3 * c + b, 0, cells) for b in range(3)] for c in range(3)]
    offset = [[row_of_cells(pair_out, 16 + 3 * a + b, 0, cells) for b in range(3)] for a in range(3)]
    moment = [[None] * 3 for _ in range(3)]
    for b in range(3):
        for a in range(3):
            n, m = (a + 1) % 3, (a + 2) % 3
            moment[a][b] = position[n] * spread[m][b] - position[m] * spread[n][b] - offset[a][b]
    return [
        pair_factor * (moment[a][b] + moment[b][a])
        for a, b in ((0, 0), (1, 1), (2, 2), (1, 2), (0, 2), (0, 1))
    ]


def advance(position, sampled, field, line, burg):
    sigma = [sampled[c] + field[c] for c in range(6)]
    pull = [sum(sigma[full_index[a][b]] * burg[b] for b in range(3)) for a in range(3)]
    force = [
        pull[1] * line[2] - pull[2] * line[1],
        pull[2] * line[0] - pull[0] * line[2],
        pull[0] * line[1] - pull[1] * line[0],
    ]
    return [position[k] + step_size * force[k] for k in range(3)]


def kernel(
    plastic_hbm, table_hbm, back_hbm, offsets_hbm, lines_hbm, burgers_hbm, counts_hbm, voxels_hbm,
    stress_out, seg_out, samp_out, field_out, lbuf, second_out, third_out,
    plastic_buf, table_buf, back_buf, offsets_ref, lines_ref, burgers_ref, counts_ref, voxels_ref,
    out1, in1, out2, in2, spec, stress_buf, seg, samp, own, mbuf, mlate, pair_out, factor_buf,
    load_sem, send1, recv1, send2, recv2, halo_send, halo_recv, samp_send, samp_recv,
):
    gx = lax.axis_index("gx")
    pa = lax.axis_index("pa")
    mode = pa * GX + gx
    left = {"gx": (gx + 7) % 8}
    right = {"gx": (gx + 1) % 8}

    def device(i):
        return {"gx": gx ^ (i & 7), "pa": pa ^ (i >> 3)}

    sources = (plastic_hbm, offsets_hbm, lines_hbm, burgers_hbm, counts_hbm, voxels_hbm, back_hbm)
    targets = (plastic_buf, offsets_ref, lines_ref, burgers_ref, counts_ref, voxels_ref, back_buf)
    loads = [
        pltpu.make_async_copy(source, target, load_sem.at[i])
        for i, (source, target) in enumerate(zip(sources, targets))
    ]
    table_loads = [
        pltpu.make_async_copy(table_hbm.at[i], table_buf.at[i], load_sem.at[len(loads) + i]) for i in range(10)
    ]
    barrier = pltpu.get_barrier_semaphore()
    with jax.named_scope("greet"):
        loads[0].start()
        table_loads[0].start()
        table_loads[1].start()
        for i in partners():
            pl.semaphore_signal(barrier, inc=1, device_id=device(i), device_id_type=MESH)
        for copy in loads[1:] + table_loads[2:]:
            copy.start()

    lane8 = lax.broadcasted_iota(jnp.int32, (8, N), 1)
    upper = jnp.where(lax.broadcasted_iota(jnp.int32, (N, N), 1) >= N // 2, -1.0, 1.0)

    def message(ref, number):
        return ref.at[pl.ds(6 * number, 6)]

    def send_all(source, target, send_sem, recv_sem):
        for i in partners():
            pltpu.make_async_remote_copy(
                src_ref=message(source, mode ^ i), dst_ref=message(target, mode),
                send_sem=send_sem, recv_sem=recv_sem, device_id=device(i), device_id_type=MESH,
            ).start()
        pltpu.make_async_copy(message(source, mode), message(target, mode), recv_sem).start()

    def wait_all(target, recv_sem):
        pltpu.make_async_copy(target, target, recv_sem).wait()

    def put(target, c, value):
        target[pl.ds(c, N, stride=6), :] = value

    def take(source, c):
        return source[pl.ds(c, N, stride=6), :]

    with jax.named_scope("wait_load"):
        loads[0].wait()
        table_loads[0].wait()
        table_loads[1].wait()
    with jax.named_scope("z_ahead"):
        for pair in PAIRS:
            rows = jnp.concatenate([plastic_buf[c].reshape(N, N) for c in pair], axis=0)
            high, low = split(rows)
            both = dot(table_buf[1 if pair[0] == 3 else 0], jnp.concatenate([high, low], axis=1), (1, 1))
            result = both[:N] + both[N:]
            put(out1, pair[0], result[:, :N])
            put(out1, pair[1], result[:, N:])
    with jax.named_scope("wait_barrier"):
        pl.semaphore_wait(barrier, N - 1)
    with jax.named_scope("send1"):
        send_all(out1, in1, send1, recv1)

    for copy in loads[1:6]:
        copy.wait()
    counts = counts_ref[...]
    index = lax.broadcasted_iota(jnp.int32, (CELLS, N), 1)
    live = (index < counts.reshape(CELLS, 1)).astype(F32)
    first_position = []
    for k in range(3):
        value = offsets_ref[k, 0] - 0.5
        seg[HALO : HALO + CELLS, k, :] = value
        seg[HALO : HALO + CELLS, 3 + k, :] = lines_ref[k, 0]
        seg[HALO : HALO + CELLS, 6 + k, :] = burgers_ref[k, 0] * live
    to_left = pltpu.make_async_remote_copy(
        src_ref=seg.at[pl.ds(HALO, HALO)], dst_ref=seg.at[pl.ds(HALO + CELLS, HALO)],
        send_sem=halo_send.at[0], recv_sem=halo_recv.at[0], device_id=left, device_id_type=MESH,
    )
    to_right = pltpu.make_async_remote_copy(
        src_ref=seg.at[pl.ds(CELLS, HALO)], dst_ref=seg.at[pl.ds(0, HALO)],
        send_sem=halo_send.at[1], recv_sem=halo_recv.at[1], device_id=right, device_id_type=MESH,
    )
    to_left.start()
    to_right.start()

    for copy in table_loads[2:]:
        copy.wait()
    loads[6].wait()
    with jax.named_scope("wait_in1"):
        wait_all(in1, recv1)
    with jax.named_scope("y_ahead"):
        for c in range(6):
            spec[c] = y_matmul(butterfly(take(in1, c), lane8), table_buf[2])
    with jax.named_scope("x_ahead"):
        for pair in PAIRS:
            table = table_buf[4 if pair[0] == 3 else 3]
            spec[pair[0]], spec[pair[1]] = x_matmul(table, spec[pair[0]], spec[pair[1]], upper)

    with jax.named_scope("operator"):
        freq_y = signed_frequency(lane8 % 64)
        freq_z = jnp.where(mode % 2 == 0, mode // 2, -(mode // 2)).astype(F32)
        for t in range(N // 8):
            freq_x = signed_frequency(lax.broadcasted_iota(jnp.int32, (8, N), 0) + 8 * t)
            strain = [spec[c, 8 * t : 8 * t + 8, :] for c in range(6)]
            result = stress_terms(strain, freq_x, freq_y, freq_z)
            for c in range(6):
                spec[c, 8 * t : 8 * t + 8, :] = result[c]

    with jax.named_scope("x_back"):
        for pair in PAIRS:
            table = table_buf[6 if pair[0] == 3 else 5]
            spec[pair[0]], spec[pair[1]] = x_matmul(table, spec[pair[0]], spec[pair[1]], upper)
    with jax.named_scope("y_back"):
        for c in range(6):
            put(out2, c, butterfly(y_matmul(spec[c], table_buf[7]), lane8))
    with jax.named_scope("send2"):
        send_all(out2, in2, send2, recv2)

    with jax.named_scope("wait_halo"):
        to_left.wait()
        to_right.wait()
    start, line, burg = ([row_of_cells(seg, 3 * i + k, 0, WIDE) for k in range(3)] for i in range(3))
    for i, part in enumerate((start, line, burg)):
        for k in range(3):
            seg_out[3 * i + k] = part[k][1 : 1 + LATE]
    with jax.named_scope("pair1"):
        lbuf[...] = jnp.zeros_like(lbuf)
        mbuf[...] = jnp.zeros_like(mbuf)
        mlate[...] = jnp.zeros_like(mlate)
        pair_out[...] = jnp.zeros_like(pair_out)
        own[...] = jnp.zeros_like(own)
        flat = lbuf.reshape(WIDE * 16, N)
        for c in range(3):
            for b in range(3):
                flat[pl.ds(3 * c + b, WIDE, stride=16), :] = line[c] * burg[b]
        arms_into(mbuf, start, line, burg)
        pair_blocks(start, lbuf, mbuf, pair_out, [(cell, (0, 1, 2)) for cell in range(1, WIDE - 1)])
        field = pair_field(start, pair_out)
        for c in range(6):
            field_out[c] = field[c][1 : 1 + LATE]
        second_out[...] = jnp.zeros_like(second_out)
        third_out[...] = jnp.zeros_like(third_out)

    voxels = voxels_ref[0]
    column_of = voxels >> 7
    z_of = voxels & 127
    with jax.named_scope("factors"):
        for cell in range(CELLS):
            pick_z = jnp.broadcast_to(z_of[cell : cell + 1], (8, N))
            for odd in range(2):
                for t in range(N // 8):
                    rows = slice(8 * t, 8 * t + 8)
                    factor_buf[cell, odd, rows] = jnp.take_along_axis(
                        back_buf[odd, rows], pick_z, axis=1, mode="promise_in_bounds"
                    )
    with jax.named_scope("wait_in2"):
        wait_all(in2, recv2)
    with jax.named_scope("sample"):
        for c in range(6):
            stress_buf[c] = take(in2, c)
        for cell in range(CELLS):
            pick = jnp.broadcast_to(column_of[cell : cell + 1], (8, N))
            total = [None] * 6
            for t in range(N // 8):
                rows = slice(8 * t, 8 * t + 8)
                factor = [factor_buf[cell, odd, rows] for odd in range(2)]
                for c in range(6):
                    tile = jnp.take_along_axis(stress_buf[c, rows], pick, axis=1, mode="promise_in_bounds")
                    term = tile * factor[1 if c in (3, 4) else 0]
                    total[c] = term if t == 0 else total[c] + term
            for c in range(6):
                value = jnp.sum(total[c], axis=0, keepdims=True)
                samp[HALO + cell, c : c + 1, :] = value
                own[HALO + cell, c : c + 1, :] = value

    samp_left = pltpu.make_async_remote_copy(
        src_ref=samp.at[pl.ds(HALO, 2)], dst_ref=samp.at[pl.ds(HALO + CELLS, 2)],
        send_sem=samp_send.at[0], recv_sem=samp_recv.at[0], device_id=left, device_id_type=MESH,
    )
    samp_right = pltpu.make_async_remote_copy(
        src_ref=samp.at[pl.ds(HALO + 2, 2)], dst_ref=samp.at[pl.ds(1, 2)],
        send_sem=samp_send.at[1], recv_sem=samp_recv.at[1], device_id=right, device_id_type=MESH,
    )
    samp_left.start()
    samp_right.start()
    with jax.named_scope("z_back"):
        for pair in PAIRS:
            table = table_buf[9 if pair[0] == 3 else 8]
            high, low = split(jnp.concatenate([stress_buf[c] for c in pair], axis=1))
            both = dot(table, jnp.concatenate([high, low], axis=0))
            result = both[:N] + both[N:]
            for c, half in zip(pair, (result[:, :N], result[:, N:])):
                stress_out[c] = jnp.transpose(half).reshape(16, 8, N)
    with jax.named_scope("pair_own"):
        start, line, burg = ([seg_out[3 * i + k] for k in range(3)] for i in range(3))
        sampled = [row_of_cells(own, c, 1, LATE) for c in range(6)]
        position = advance(start, sampled, [field_out[c] for c in range(6)], line, burg)
        arms_into(mlate, position, line, burg)
        pair_blocks(position, lbuf, mlate, second_out, OWN_SECOND)
        position = advance(position, sampled, pair_field(position, second_out), line, burg)
        arms_into(mlate, position, line, burg)
        pair_blocks(position, lbuf, mlate, third_out, OWN_THIRD)

    with jax.named_scope("wait_samp"):
        samp_left.wait()
        samp_right.wait()
    for c in range(6):
        samp_out[c] = row_of_cells(samp, c, 1, LATE)

    for source, send_sem in ((out1, send1), (out2, send2)):
        sent = source.at[pl.ds(0, 6 * (N - 1))]
        pltpu.make_async_copy(sent, sent, send_sem).wait()


def finish(
    stress_ref, seg, samp, field_ref, lbuf, second, third, stress_hbm, moved_hbm,
    mbuf, second_buf, third_buf, moved_ref, store_sem,
):
    store = pltpu.make_async_copy(stress_ref, stress_hbm, store_sem.at[0])
    store.start()
    start, line, burg = ([seg[3 * i + k] for k in range(3)] for i in range(3))
    sampled = [samp[c] for c in range(6)]
    for cell in (0, 3, 4, 7):
        second_buf[cell] = second[cell]
    for cell in (0, 1, 6, 7):
        third_buf[cell] = third[cell]
    with jax.named_scope("pair_second"):
        position = advance(start, sampled, [field_ref[c] for c in range(6)], line, burg)
        arms_into(mbuf, position, line, burg)
        pair_blocks(position, lbuf, mbuf, second_buf, REST_SECOND, second)
    with jax.named_scope("pair_third"):
        position = advance(position, sampled, pair_field(position, second_buf), line, burg)
        arms_into(mbuf, position, line, burg)
        pair_blocks(position, lbuf, mbuf, third_buf, REST_THIRD, third)
    with jax.named_scope("last"):
        position = advance(position, sampled, pair_field(position, third_buf), line, burg)
        for k in range(3):
            moved_ref[k, 0] = (position[k] - start[k])[2 : 2 + CELLS]
    moved_store = pltpu.make_async_copy(moved_ref, moved_hbm, store_sem.at[1])
    moved_store.start()
    store.wait()
    moved_store.wait()


def body(plastic, offsets, lines, burgers, counts, voxels):
    any_space = pl.BlockSpec(memory_space=pl.ANY)
    dma = pltpu.SemaphoreType.DMA
    group = pltpu.VMEM((6 * N, N), F32)
    vectors = pltpu.VMEM((3, 1, CELLS, N), F32)
    table, back = tables()
    vmem = pl.BlockSpec(memory_space=pltpu.VMEM)
    state = pl.pallas_call(
        kernel,
        out_shape=(
            pltpu.VMEM((6, 16, 8, N), F32),
            pltpu.VMEM((9, LATE, N), F32),
            pltpu.VMEM((6, LATE, N), F32),
            pltpu.VMEM((6, LATE, N), F32),
            pltpu.VMEM((WIDE, 16, N), F32),
            pltpu.VMEM((LATE, 32, N), F32),
            pltpu.VMEM((LATE, 32, N), F32),
        ),
        in_specs=[any_space] * 8,
        out_specs=(vmem,) * 7,
        scratch_shapes=[
            pltpu.VMEM((6, 16, 8, N), F32),
            pltpu.VMEM((10, 2 * N, 2 * N), BF16),
            pltpu.VMEM((2, N, N), F32),
            vectors, vectors, vectors,
            pltpu.VMEM((1, CELLS), jnp.int32),
            pltpu.VMEM((1, CELLS, N), jnp.int32),
            group, group, group, group,
            pltpu.VMEM((6, N, N), F32),
            pltpu.VMEM((6, N, N), F32),
            pltpu.VMEM((WIDE, 16, N), F32),
            pltpu.VMEM((WIDE, 8, N), F32),
            pltpu.VMEM((WIDE, 8, N), F32),
            pltpu.VMEM((3, WIDE, 16, N), F32),
            pltpu.VMEM((3, LATE, 16, N), F32),
            pltpu.VMEM((WIDE, 32, N), F32),
            pltpu.VMEM((CELLS, 2, N, N), F32),
            dma((17,)),
            dma, dma, dma, dma,
            dma((2,)), dma((2,)), dma((2,)), dma((2,)),
        ],
        compiler_params=pltpu.CompilerParams(collective_id=0, has_side_effects=True),
    )(plastic, jnp.asarray(table), jnp.asarray(back), offsets, lines, burgers, counts, voxels)
    return pl.pallas_call(
        finish,
        out_shape=(
            jax.ShapeDtypeStruct((6, 16, 8, N), F32),
            jax.ShapeDtypeStruct((3, 1, CELLS, N), F32),
        ),
        in_specs=[vmem] * 7,
        out_specs=(any_space, any_space),
        scratch_shapes=[
            pltpu.VMEM((3, LATE, 16, N), F32),
            pltpu.VMEM((LATE, 32, N), F32),
            pltpu.VMEM((LATE, 32, N), F32),
            vectors,
            dma((2,)),
        ],
    )(*[pltpu.with_memory_space_constraint(array, pltpu.VMEM) for array in state])


def solution(mesh):
    placed = (
        P(None, "gx", "pa", None),
        P(None, "pa", "gx", None),
        P(None, "pa", "gx", None),
        P(None, "pa", "gx", None),
        P("pa", "gx"),
        P("pa", "gx", None),
    )
    return jax.shard_map(
        body,
        mesh=mesh,
        in_specs=placed,
        out_specs=(P(None, "gx", "pa", None), P(None, "pa", "gx", None)),
        check_vma=False,
    )
```

```python
import math

import jax
import jax.numpy as jnp
import numpy as np
from jax import lax
from jax.experimental import pallas as pl
from jax.experimental.pallas import tpu as pltpu
from jax.sharding import PartitionSpec as P

MESH = pl.DeviceIdType.MESH
F32 = jnp.float32
BF16 = jnp.bfloat16
N = 128
GX = 8
PA = 16
PAIRS = ((0, 1), (2, 5), (3, 4))
CELLS = 4
HALO = 3
WIDE = CELLS + 2 * HALO
LATE = 8
OWN_SECOND = ((2, (1, 2)), (3, (0, 1, 2)), (4, (0, 1, 2)), (5, (0, 1)))
REST_SECOND = ((1, (0, 1, 2)), (2, (0,)), (5, (2,)), (6, (0, 1, 2)))
OWN_THIRD = ((3, (1, 2)), (4, (0, 1)))
REST_THIRD = ((2, (0, 1, 2)), (3, (0,)), (4, (2,)), (5, (0, 1, 2)))

lame_lambda = 1.5
shear_modulus = 1.0
green_coef = 2.5 / 3.5
core_square = 0.09
pair_factor = 1.0 / (4.0 * math.pi)
step_size = 0.05
full_index = ((0, 5, 4), (5, 1, 3), (4, 3, 2))


def np_split(table):
    table = np.asarray(table, np.float32)
    high = table.astype(jnp.bfloat16)
    low = (table - high.astype(np.float32)).astype(jnp.bfloat16)
    return high, low


def tables():
    index = np.arange(N)
    angle = 2.0 * np.pi * (np.outer(index, index) % N) / N
    cos, sin = np.cos(angle), np.sin(angle)
    flip = np.where(index % 2 == 0, 1.0, -1.0)
    bins, parity = index // 2, index % 2
    weight = np.where(bins == 0, 1.0, 2.0)[:, None] / N
    ahead_z = []
    for odd in range(2):
        imaginary = (parity == 1 - odd)[:, None]
        table = np.where(imaginary, -sin[bins], cos[bins])
        ahead_z.append(np.where(imaginary & (bins == 0)[:, None], flip[None, :], table))
    back_z = [table * weight for table in ahead_z]
    ky = np.arange(N // 2)
    ahead_y = np.concatenate([cos[:, ky], -sin[:, ky]], axis=1)
    ahead_y[:, N // 2] = flip
    back_y = ahead_y.T * np.where(index % 64 == 0, 1.0, 2.0)[:, None] / N
    plane = (index % 8) * 16 + index // 8
    cx, sx = cos[:, plane], sin[:, plane]
    ahead_x = [np.concatenate([cx, sx], axis=1), np.concatenate([sx, -cx], axis=1)]
    back_x = [np.concatenate([cx.T, -sx.T], axis=1) / N, np.concatenate([sx.T, cx.T], axis=1) / N]

    def beside(table):
        high, low = np_split(table)
        return np.block([[high, high], [low, np.zeros_like(low)]])

    def under(table):
        high, low = np_split(table)
        return np.block([[high, low], [high, np.zeros_like(low)]])

    def stacked(table):
        return np.concatenate(np_split(table), axis=0)

    out = [beside(ahead_z[0]), beside(ahead_z[1]), under(ahead_y)]
    out += [stacked(ahead_x[0]), stacked(ahead_x[1]), stacked(back_x[0]), stacked(back_x[1])]
    out += [under(back_y), beside(back_z[0].T), beside(back_z[1].T)]
    return np.stack(out), np.stack(back_z).astype(np.float32)


def split(value):
    high = value.astype(BF16)
    low = (value - high.astype(F32)).astype(BF16)
    return high, low


def dot(a, b, contract=(1, 0)):
    return lax.dot_general(a, b, (((contract[0],), (contract[1],)), ((), ())), preferred_element_type=F32)


def butterfly(value, lane):
    tiles = [value[8 * t : 8 * t + 8] for t in range(PA)]
    for step in (4, 1):
        low = (lane & (step * 8)) != 0
        high = (lane & (step * 16)) != 0

        def by_digit(options):
            return jnp.where(high, jnp.where(low, options[3], options[2]), jnp.where(low, options[1], options[0]))

        for base in range(PA):
            if base & (3 * step):
                continue
            held = [tiles[base + step * t] for t in range(4)]
            gone = [None] * 4
            for d in range(1, 4):
                going = by_digit([held[u ^ d] for u in range(4)])
                if d * step * 8 == N // 2:
                    gone[d] = pltpu.roll(going, N // 2, 1)
                else:
                    gone[d] = jnp.take_along_axis(going, lane ^ (d * step * 8), axis=1, mode="promise_in_bounds")
            for t in range(4):
                tiles[base + step * t] = by_digit([held[t] if g == t else gone[g ^ t] for g in range(4)])
    return jnp.concatenate(tiles, axis=0)


def turned(value, sign):
    return pltpu.roll(value, N // 2, 1) * sign


def y_matmul(rows, table):
    high, low = split(rows)
    both = dot(jnp.concatenate([high, low], axis=1), table)
    return both[:, :N] + both[:, N:]


def x_matmul(table, first, second, upper):
    top = jnp.concatenate([first, second], axis=1)
    below = jnp.concatenate([turned(first, upper), turned(second, upper)], axis=1)
    high, low = split(jnp.concatenate([top, below], axis=0))
    both = dot(table, high)
    result = both[:N] + both[N:] + dot(table[:N], low)
    return result[:, :N], result[:, N:]


def stress_terms(strain, freq_x, freq_y, freq_z):
    xx, yy, zz, yz, xz, xy = strain
    trace = xx + yy + zz
    tau_xx = lame_lambda * trace + 2.0 * shear_modulus * xx
    tau_yy = lame_lambda * trace + 2.0 * shear_modulus * yy
    tau_zz = lame_lambda * trace + 2.0 * shear_modulus * zz
    tau_yz = 2.0 * shear_modulus * yz
    tau_xz = 2.0 * shear_modulus * xz
    tau_xy = 2.0 * shear_modulus * xy
    norm_x = tau_xx * freq_x + tau_xy * freq_y + tau_xz * freq_z
    norm_y = tau_xy * freq_x + tau_yy * freq_y + tau_yz * freq_z
    norm_z = tau_xz * freq_x + tau_yz * freq_y + tau_zz * freq_z
    square = freq_x * freq_x + freq_y * freq_y + freq_z * freq_z
    inverse = 1.0 / jnp.maximum(square, 1.0)
    along = (freq_x * norm_x + freq_y * norm_y + freq_z * norm_z) * inverse * inverse * green_coef
    half = inverse / (2.0 * shear_modulus)

    def term(first_q, second_q, first_n, second_n, plastic):
        total = (first_q * second_n + second_q * first_n) * half - first_q * second_q * along
        return total - plastic

    el_xx = term(freq_x, freq_x, norm_x, norm_x, xx)
    el_yy = term(freq_y, freq_y, norm_y, norm_y, yy)
    el_zz = term(freq_z, freq_z, norm_z, norm_z, zz)
    el_yz = term(freq_y, freq_z, norm_y, norm_z, yz)
    el_xz = term(freq_x, freq_z, norm_x, norm_z, xz)
    el_xy = term(freq_x, freq_y, norm_x, norm_y, xy)
    el_trace = el_xx + el_yy + el_zz
    return (
        lame_lambda * el_trace + 2.0 * shear_modulus * el_xx,
        lame_lambda * el_trace + 2.0 * shear_modulus * el_yy,
        lame_lambda * el_trace + 2.0 * shear_modulus * el_zz,
        2.0 * shear_modulus * el_yz,
        2.0 * shear_modulus * el_xz,
        2.0 * shear_modulus * el_xy,
    )


SEND_COST = ((0.0, 0.6, 1.5, 1.0), (0.0, 1.0, 2.3, 1.6), (0.0, 1.5, 3.6, 2.4))
GREET_COST = ((0.0, 1.0, 2.0, 2.4),) * 3


def partners(cost):
    def distance(i):
        return cost[0][2 * (i >> 6) + (i & 1)] + cost[1][(i & 7) >> 1] + cost[2][(i >> 4) & 3]

    return sorted(range(1, N), key=lambda i: -distance(i))


def signed_frequency(index):
    value = jnp.where(index < N // 2, index, jnp.where(index == N // 2, 0, index - N))
    return value.astype(F32)


def row_of_cells(ref, row, first, count):
    cells, rows = ref.shape[0], ref.shape[1]
    return ref.reshape(cells * rows, N)[pl.ds(first * rows + row, count, stride=rows), :]


def arms_into(mbuf, position, line, burg):
    cells = position[0].shape[0]
    flat = mbuf.reshape(3 * mbuf.shape[1] * 16, N)
    arm = [
        position[1] * line[2] - position[2] * line[1],
        position[2] * line[0] - position[0] * line[2],
        position[0] * line[1] - position[1] * line[0],
    ]
    for shift in range(3):
        moved_arm = [
            arm[0],
            arm[1] - (shift - 1.0) * line[2],
            arm[2] + (shift - 1.0) * line[1],
        ]
        for a in range(3):
            for b in range(3):
                at = shift * mbuf.shape[1] * 16 + 3 * a + b
                flat[pl.ds(at, cells, stride=16), :] = moved_arm[a] * burg[b]


def pair_blocks(position, lbuf, mbuf, pair_out, blocks, before=None):
    cells = position[0].shape[0]
    extra = (WIDE - cells) // 2
    if cells % 8:
        pad = jnp.zeros((16 - cells, N), F32)
        columns = [jnp.transpose(jnp.concatenate([value, pad], axis=0)) for value in position]
    else:
        columns = [jnp.transpose(value) for value in position]
    for cell, shifts in blocks:
        target = [value[cell : cell + 1] for value in position]
        weights, factors = [], []
        for shift in shifts:
            source = cell + shift - 1
            delta = [
                (target[k] - (shift - 1.0) * (k == 0)) - columns[k][:, source : source + 1] for k in range(3)
            ]
            radius = delta[0] * delta[0] + delta[1] * delta[1] + delta[2] * delta[2] + core_square
            root = lax.rsqrt(radius)
            weights.append(root * root * root)
            factors.append(jnp.concatenate([lbuf[source + extra], mbuf[shift, source]], axis=0))
        weight_high, weight_low = split(jnp.concatenate(weights, axis=0))
        factor_high, factor_low = split(jnp.concatenate(factors, axis=1))
        both = dot(jnp.concatenate([factor_high, factor_low], axis=0), weight_high)
        total = both[:32] + both[32:] + dot(factor_high, weight_low)
        if before is not None and len(shifts) < 3:
            total = total + before[cell]
        pair_out[cell] = total


def pair_field(position, pair_out):
    cells = position[0].shape[0]
    spread = [[row_of_cells(pair_out, 3 * c + b, 0, cells) for b in range(3)] for c in range(3)]
    offset = [[row_of_cells(pair_out, 16 + 3 * a + b, 0, cells) for b in range(3)] for a in range(3)]
    moment = [[None] * 3 for _ in range(3)]
    for b in range(3):
        for a in range(3):
            n, m = (a + 1) % 3, (a + 2) % 3
            moment[a][b] = position[n] * spread[m][b] - position[m] * spread[n][b] - offset[a][b]
    return [
        pair_factor * (moment[a][b] + moment[b][a])
        for a, b in ((0, 0), (1, 1), (2, 2), (1, 2), (0, 2), (0, 1))
    ]


def advance(position, sampled, field, line, burg):
    sigma = [sampled[c] + field[c] for c in range(6)]
    pull = [sum(sigma[full_index[a][b]] * burg[b] for b in range(3)) for a in range(3)]
    force = [
        pull[1] * line[2] - pull[2] * line[1],
        pull[2] * line[0] - pull[0] * line[2],
        pull[0] * line[1] - pull[1] * line[0],
    ]
    return [position[k] + step_size * force[k] for k in range(3)]


def kernel(
    plastic_hbm, table_hbm, back_hbm, offsets_hbm, lines_hbm, burgers_hbm, counts_hbm, voxels_hbm,
    stress_out, seg_out, samp_out, field_out, lbuf, second_out, third_out,
    plastic_buf, table_buf, back_buf, offsets_ref, lines_ref, burgers_ref, counts_ref, voxels_ref,
    out1, in1, out2, in2, spec, stress_buf, seg, samp, own, mbuf, mlate, pair_out, factor_buf,
    load_sem, send1, recv1, send2, recv2, halo_send, halo_recv, samp_send, samp_recv,
):
    gx = lax.axis_index("gx")
    pa = lax.axis_index("pa")
    mode = pa * GX + gx
    left = {"gx": (gx + 7) % 8}
    right = {"gx": (gx + 1) % 8}

    def device(i):
        return {"gx": gx ^ (i & 7), "pa": pa ^ (i >> 3)}

    sources = (plastic_hbm, offsets_hbm, lines_hbm, burgers_hbm, counts_hbm, voxels_hbm, back_hbm)
    targets = (plastic_buf, offsets_ref, lines_ref, burgers_ref, counts_ref, voxels_ref, back_buf)
    loads = [
        pltpu.make_async_copy(source, target, load_sem.at[i])
        for i, (source, target) in enumerate(zip(sources, targets))
    ]
    table_loads = [
        pltpu.make_async_copy(table_hbm.at[i], table_buf.at[i], load_sem.at[len(loads) + i]) for i in range(10)
    ]
    barrier = pltpu.get_barrier_semaphore()
    with jax.named_scope("greet"):
        loads[0].start()
        table_loads[0].start()
        table_loads[1].start()
        for i in partners(GREET_COST):
            pl.semaphore_signal(barrier, inc=1, device_id=device(i), device_id_type=MESH)
        for copy in loads[1:] + table_loads[2:]:
            copy.start()

    lane8 = lax.broadcasted_iota(jnp.int32, (8, N), 1)
    upper = jnp.where(lax.broadcasted_iota(jnp.int32, (N, N), 1) >= N // 2, -1.0, 1.0)

    def message(ref, number):
        return ref.at[pl.ds(6 * number, 6)]

    def send_all(source, target, send_sem, recv_sem):
        for i in partners(SEND_COST):
            pltpu.make_async_remote_copy(
                src_ref=message(source, mode ^ i), dst_ref=message(target, mode),
                send_sem=send_sem, recv_sem=recv_sem, device_id=device(i), device_id_type=MESH,
            ).start()
        pltpu.make_async_copy(message(source, mode), message(target, mode), recv_sem).start()

    def wait_all(target, recv_sem):
        pltpu.make_async_copy(target, target, recv_sem).wait()

    def put(target, c, value):
        target[pl.ds(c, N, stride=6), :] = value

    def take(source, c):
        return source[pl.ds(c, N, stride=6), :]

    with jax.named_scope("wait_load"):
        loads[0].wait()
        table_loads[0].wait()
        table_loads[1].wait()
    with jax.named_scope("z_ahead"):
        for pair in PAIRS:
            rows = jnp.concatenate([plastic_buf[c].reshape(N, N) for c in pair], axis=0)
            high, low = split(rows)
            both = dot(table_buf[1 if pair[0] == 3 else 0], jnp.concatenate([high, low], axis=1), (1, 1))
            result = both[:N] + both[N:]
            put(out1, pair[0], result[:, :N])
            put(out1, pair[1], result[:, N:])
    with jax.named_scope("wait_barrier"):
        pl.semaphore_wait(barrier, N - 1)
    with jax.named_scope("send1"):
        send_all(out1, in1, send1, recv1)

    for copy in loads[1:6]:
        copy.wait()
    counts = counts_ref[...]
    index = lax.broadcasted_iota(jnp.int32, (CELLS, N), 1)
    live = (index < counts.reshape(CELLS, 1)).astype(F32)
    first_position = []
    for k in range(3):
        value = offsets_ref[k, 0] - 0.5
        seg[HALO : HALO + CELLS, k, :] = value
        seg[HALO : HALO + CELLS, 3 + k, :] = lines_ref[k, 0]
        seg[HALO : HALO + CELLS, 6 + k, :] = burgers_ref[k, 0] * live
    to_left = pltpu.make_async_remote_copy(
        src_ref=seg.at[pl.ds(HALO, HALO)], dst_ref=seg.at[pl.ds(HALO + CELLS, HALO)],
        send_sem=halo_send.at[0], recv_sem=halo_recv.at[0], device_id=left, device_id_type=MESH,
    )
    to_right = pltpu.make_async_remote_copy(
        src_ref=seg.at[pl.ds(CELLS, HALO)], dst_ref=seg.at[pl.ds(0, HALO)],
        send_sem=halo_send.at[1], recv_sem=halo_recv.at[1], device_id=right, device_id_type=MESH,
    )
    to_left.start()
    to_right.start()

    for copy in table_loads[2:]:
        copy.wait()
    loads[6].wait()
    with jax.named_scope("wait_in1"):
        wait_all(in1, recv1)
    with jax.named_scope("y_ahead"):
        for c in range(6):
            spec[c] = y_matmul(butterfly(take(in1, c), lane8), table_buf[2])
    with jax.named_scope("x_ahead"):
        for pair in PAIRS:
            table = table_buf[4 if pair[0] == 3 else 3]
            spec[pair[0]], spec[pair[1]] = x_matmul(table, spec[pair[0]], spec[pair[1]], upper)

    with jax.named_scope("operator"):
        freq_y = signed_frequency(lane8 % 64)
        freq_z = jnp.where(mode % 2 == 0, mode // 2, -(mode // 2)).astype(F32)
        for t in range(N // 8):
            freq_x = signed_frequency(lax.broadcasted_iota(jnp.int32, (8, N), 0) + 8 * t)
            strain = [spec[c, 8 * t : 8 * t + 8, :] for c in range(6)]
            result = stress_terms(strain, freq_x, freq_y, freq_z)
            for c in range(6):
                spec[c, 8 * t : 8 * t + 8, :] = result[c]

    with jax.named_scope("x_back"):
        for pair in PAIRS:
            table = table_buf[6 if pair[0] == 3 else 5]
            spec[pair[0]], spec[pair[1]] = x_matmul(table, spec[pair[0]], spec[pair[1]], upper)
    with jax.named_scope("y_back"):
        for c in range(6):
            put(out2, c, butterfly(y_matmul(spec[c], table_buf[7]), lane8))
    with jax.named_scope("send2"):
        send_all(out2, in2, send2, recv2)

    with jax.named_scope("wait_halo"):
        to_left.wait()
        to_right.wait()
    start, line, burg = ([row_of_cells(seg, 3 * i + k, 0, WIDE) for k in range(3)] for i in range(3))
    for i, part in enumerate((start, line, burg)):
        for k in range(3):
            seg_out[3 * i + k] = part[k][1 : 1 + LATE]
    with jax.named_scope("pair1"):
        lbuf[...] = jnp.zeros_like(lbuf)
        mbuf[...] = jnp.zeros_like(mbuf)
        mlate[...] = jnp.zeros_like(mlate)
        pair_out[...] = jnp.zeros_like(pair_out)
        own[...] = jnp.zeros_like(own)
        flat = lbuf.reshape(WIDE * 16, N)
        for c in range(3):
            for b in range(3):
                flat[pl.ds(3 * c + b, WIDE, stride=16), :] = line[c] * burg[b]
        arms_into(mbuf, start, line, burg)
        pair_blocks(start, lbuf, mbuf, pair_out, [(cell, (0, 1, 2)) for cell in range(1, WIDE - 1)])
        field = pair_field(start, pair_out)
        for c in range(6):
            field_out[c] = field[c][1 : 1 + LATE]
        second_out[...] = jnp.zeros_like(second_out)
        third_out[...] = jnp.zeros_like(third_out)

    voxels = voxels_ref[0]
    column_of = voxels >> 7
    z_of = voxels & 127
    with jax.named_scope("factors"):
        for cell in range(CELLS):
            pick_z = jnp.broadcast_to(z_of[cell : cell + 1], (8, N))
            for odd in range(2):
                for t in range(N // 8):
                    rows = slice(8 * t, 8 * t + 8)
                    factor_buf[cell, odd, rows] = jnp.take_along_axis(
                        back_buf[odd, rows], pick_z, axis=1, mode="promise_in_bounds"
                    )
    with jax.named_scope("wait_in2"):
        wait_all(in2, recv2)
    with jax.named_scope("sample"):
        for c in range(6):
            stress_buf[c] = take(in2, c)
        for cell in range(CELLS):
            pick = jnp.broadcast_to(column_of[cell : cell + 1], (8, N))
            total = [None] * 6
            for t in range(N // 8):
                rows = slice(8 * t, 8 * t + 8)
                factor = [factor_buf[cell, odd, rows] for odd in range(2)]
                for c in range(6):
                    tile = jnp.take_along_axis(stress_buf[c, rows], pick, axis=1, mode="promise_in_bounds")
                    term = tile * factor[1 if c in (3, 4) else 0]
                    total[c] = term if t == 0 else total[c] + term
            for c in range(6):
                value = jnp.sum(total[c], axis=0, keepdims=True)
                samp[HALO + cell, c : c + 1, :] = value
                own[HALO + cell, c : c + 1, :] = value

    samp_left = pltpu.make_async_remote_copy(
        src_ref=samp.at[pl.ds(HALO, 2)], dst_ref=samp.at[pl.ds(HALO + CELLS, 2)],
        send_sem=samp_send.at[0], recv_sem=samp_recv.at[0], device_id=left, device_id_type=MESH,
    )
    samp_right = pltpu.make_async_remote_copy(
        src_ref=samp.at[pl.ds(HALO + 2, 2)], dst_ref=samp.at[pl.ds(1, 2)],
        send_sem=samp_send.at[1], recv_sem=samp_recv.at[1], device_id=right, device_id_type=MESH,
    )
    samp_left.start()
    samp_right.start()
    with jax.named_scope("z_back"):
        for pair in PAIRS:
            table = table_buf[9 if pair[0] == 3 else 8]
            high, low = split(jnp.concatenate([stress_buf[c] for c in pair], axis=1))
            both = dot(table, jnp.concatenate([high, low], axis=0))
            result = both[:N] + both[N:]
            for c, half in zip(pair, (result[:, :N], result[:, N:])):
                stress_out[c] = jnp.transpose(half).reshape(16, 8, N)
    with jax.named_scope("pair_own"):
        start, line, burg = ([seg_out[3 * i + k] for k in range(3)] for i in range(3))
        sampled = [row_of_cells(own, c, 1, LATE) for c in range(6)]
        position = advance(start, sampled, [field_out[c] for c in range(6)], line, burg)
        arms_into(mlate, position, line, burg)
        pair_blocks(position, lbuf, mlate, second_out, OWN_SECOND)
        position = advance(position, sampled, pair_field(position, second_out), line, burg)
        arms_into(mlate, position, line, burg)
        pair_blocks(position, lbuf, mlate, third_out, OWN_THIRD)

    with jax.named_scope("wait_samp"):
        samp_left.wait()
        samp_right.wait()
    for c in range(6):
        samp_out[c] = row_of_cells(samp, c, 1, LATE)

    for source, send_sem in ((out1, send1), (out2, send2)):
        sent = source.at[pl.ds(0, 6 * (N - 1))]
        pltpu.make_async_copy(sent, sent, send_sem).wait()


def finish(
    stress_ref, seg, samp, field_ref, lbuf, second, third, stress_hbm, moved_hbm,
    mbuf, second_buf, third_buf, moved_ref, store_sem,
):
    store = pltpu.make_async_copy(stress_ref, stress_hbm, store_sem.at[0])
    store.start()
    start, line, burg = ([seg[3 * i + k] for k in range(3)] for i in range(3))
    sampled = [samp[c] for c in range(6)]
    for cell in (0, 3, 4, 7):
        second_buf[cell] = second[cell]
    for cell in (0, 1, 6, 7):
        third_buf[cell] = third[cell]
    with jax.named_scope("pair_second"):
        position = advance(start, sampled, [field_ref[c] for c in range(6)], line, burg)
        arms_into(mbuf, position, line, burg)
        pair_blocks(position, lbuf, mbuf, second_buf, REST_SECOND, second)
    with jax.named_scope("pair_third"):
        position = advance(position, sampled, pair_field(position, second_buf), line, burg)
        arms_into(mbuf, position, line, burg)
        pair_blocks(position, lbuf, mbuf, third_buf, REST_THIRD, third)
    with jax.named_scope("last"):
        position = advance(position, sampled, pair_field(position, third_buf), line, burg)
        for k in range(3):
            moved_ref[k, 0] = (position[k] - start[k])[2 : 2 + CELLS]
    moved_store = pltpu.make_async_copy(moved_ref, moved_hbm, store_sem.at[1])
    moved_store.start()
    store.wait()
    moved_store.wait()


def body(plastic, offsets, lines, burgers, counts, voxels):
    any_space = pl.BlockSpec(memory_space=pl.ANY)
    dma = pltpu.SemaphoreType.DMA
    group = pltpu.VMEM((6 * N, N), F32)
    vectors = pltpu.VMEM((3, 1, CELLS, N), F32)
    table, back = tables()
    vmem = pl.BlockSpec(memory_space=pltpu.VMEM)
    state = pl.pallas_call(
        kernel,
        out_shape=(
            pltpu.VMEM((6, 16, 8, N), F32),
            pltpu.VMEM((9, LATE, N), F32),
            pltpu.VMEM((6, LATE, N), F32),
            pltpu.VMEM((6, LATE, N), F32),
            pltpu.VMEM((WIDE, 16, N), F32),
            pltpu.VMEM((LATE, 32, N), F32),
            pltpu.VMEM((LATE, 32, N), F32),
        ),
        in_specs=[any_space] * 8,
        out_specs=(vmem,) * 7,
        scratch_shapes=[
            pltpu.VMEM((6, 16, 8, N), F32),
            pltpu.VMEM((10, 2 * N, 2 * N), BF16),
            pltpu.VMEM((2, N, N), F32),
            vectors, vectors, vectors,
            pltpu.VMEM((1, CELLS), jnp.int32),
            pltpu.VMEM((1, CELLS, N), jnp.int32),
            group, group, group, group,
            pltpu.VMEM((6, N, N), F32),
            pltpu.VMEM((6, N, N), F32),
            pltpu.VMEM((WIDE, 16, N), F32),
            pltpu.VMEM((WIDE, 8, N), F32),
            pltpu.VMEM((WIDE, 8, N), F32),
            pltpu.VMEM((3, WIDE, 16, N), F32),
            pltpu.VMEM((3, LATE, 16, N), F32),
            pltpu.VMEM((WIDE, 32, N), F32),
            pltpu.VMEM((CELLS, 2, N, N), F32),
            dma((17,)),
            dma, dma, dma, dma,
            dma((2,)), dma((2,)), dma((2,)), dma((2,)),
        ],
        compiler_params=pltpu.CompilerParams(collective_id=0, has_side_effects=True),
    )(plastic, jnp.asarray(table), jnp.asarray(back), offsets, lines, burgers, counts, voxels)
    return pl.pallas_call(
        finish,
        out_shape=(
            jax.ShapeDtypeStruct((6, 16, 8, N), F32),
            jax.ShapeDtypeStruct((3, 1, CELLS, N), F32),
        ),
        in_specs=[vmem] * 7,
        out_specs=(any_space, any_space),
        scratch_shapes=[
            pltpu.VMEM((3, LATE, 16, N), F32),
            pltpu.VMEM((LATE, 32, N), F32),
            pltpu.VMEM((LATE, 32, N), F32),
            vectors,
            dma((2,)),
        ],
    )(*[pltpu.with_memory_space_constraint(array, pltpu.VMEM) for array in state])


def solution(mesh):
    placed = (
        P(None, "gx", "pa", None),
        P(None, "pa", "gx", None),
        P(None, "pa", "gx", None),
        P(None, "pa", "gx", None),
        P("pa", "gx"),
        P("pa", "gx", None),
    )
    return jax.shard_map(
        body,
        mesh=mesh,
        in_specs=placed,
        out_specs=(P(None, "gx", "pa", None), P(None, "pa", "gx", None)),
        check_vma=False,
    )
```

```python
import math

import jax
import jax.numpy as jnp
import numpy as np
from jax import lax
from jax.experimental import pallas as pl
from jax.experimental.pallas import tpu as pltpu
from jax.sharding import PartitionSpec as P

MESH = pl.DeviceIdType.MESH
F32 = jnp.float32
BF16 = jnp.bfloat16
N = 128
GX = 8
PA = 16
PAIRS = ((0, 1), (2, 5), (3, 4))
CELLS = 4
HALO = 3
WIDE = CELLS + 2 * HALO
LATE = 8
OWN_SECOND = ((2, (1, 2)), (3, (0, 1, 2)), (4, (0, 1, 2)), (5, (0, 1)))
REST_SECOND = ((1, (0, 1, 2)), (2, (0,)), (5, (2,)), (6, (0, 1, 2)))
OWN_THIRD = ((3, (1, 2)), (4, (0, 1)))
REST_THIRD = ((2, (0, 1, 2)), (3, (0,)), (4, (2,)), (5, (0, 1, 2)))

lame_lambda = 1.5
shear_modulus = 1.0
green_coef = 2.5 / 3.5
core_square = 0.09
pair_factor = 1.0 / (4.0 * math.pi)
step_size = 0.05
full_index = ((0, 5, 4), (5, 1, 3), (4, 3, 2))


def np_split(table):
    table = np.asarray(table, np.float32)
    high = table.astype(jnp.bfloat16)
    low = (table - high.astype(np.float32)).astype(jnp.bfloat16)
    return high, low


def tables():
    index = np.arange(N)
    angle = 2.0 * np.pi * (np.outer(index, index) % N) / N
    cos, sin = np.cos(angle), np.sin(angle)
    flip = np.where(index % 2 == 0, 1.0, -1.0)
    bins, parity = index // 2, index % 2
    weight = np.where(bins == 0, 1.0, 2.0)[:, None] / N
    ahead_z = []
    for odd in range(2):
        imaginary = (parity == 1 - odd)[:, None]
        table = np.where(imaginary, -sin[bins], cos[bins])
        ahead_z.append(np.where(imaginary & (bins == 0)[:, None], flip[None, :], table))
    back_z = [table * weight for table in ahead_z]
    ky = np.arange(N // 2)
    ahead_y = np.concatenate([cos[:, ky], -sin[:, ky]], axis=1)
    ahead_y[:, N // 2] = flip
    back_y = ahead_y.T * np.where(index % 64 == 0, 1.0, 2.0)[:, None] / N
    plane = (index % 8) * 16 + index // 8
    cx, sx = cos[:, plane], sin[:, plane]
    ahead_x = [np.concatenate([cx, sx], axis=1), np.concatenate([sx, -cx], axis=1)]
    back_x = [np.concatenate([cx.T, -sx.T], axis=1) / N, np.concatenate([sx.T, cx.T], axis=1) / N]

    def beside(table):
        high, low = np_split(table)
        return np.block([[high, high], [low, np.zeros_like(low)]])

    def under(table):
        high, low = np_split(table)
        return np.block([[high, low], [high, np.zeros_like(low)]])

    def stacked(table):
        return np.concatenate(np_split(table), axis=0)

    out = [beside(ahead_z[0]), beside(ahead_z[1]), under(ahead_y)]
    out += [stacked(ahead_x[0]), stacked(ahead_x[1]), stacked(back_x[0]), stacked(back_x[1])]
    out += [under(back_y), beside(back_z[0].T), beside(back_z[1].T)]
    return np.stack(out), np.stack(back_z).astype(np.float32)


def split(value):
    high = value.astype(BF16)
    low = (value - high.astype(F32)).astype(BF16)
    return high, low


def dot(a, b, contract=(1, 0)):
    return lax.dot_general(a, b, (((contract[0],), (contract[1],)), ((), ())), preferred_element_type=F32)


def butterfly(value, lane):
    tiles = [value[8 * t : 8 * t + 8] for t in range(PA)]
    for step in (4, 1):
        low = (lane & (step * 8)) != 0
        high = (lane & (step * 16)) != 0

        def by_digit(options):
            return jnp.where(high, jnp.where(low, options[3], options[2]), jnp.where(low, options[1], options[0]))

        for base in range(PA):
            if base & (3 * step):
                continue
            held = [tiles[base + step * t] for t in range(4)]
            gone = [None] * 4
            for d in range(1, 4):
                going = by_digit([held[u ^ d] for u in range(4)])
                if d * step * 8 == N // 2:
                    gone[d] = pltpu.roll(going, N // 2, 1)
                else:
                    gone[d] = jnp.take_along_axis(going, lane ^ (d * step * 8), axis=1, mode="promise_in_bounds")
            for t in range(4):
                tiles[base + step * t] = by_digit([held[t] if g == t else gone[g ^ t] for g in range(4)])
    return jnp.concatenate(tiles, axis=0)


def turned(value, sign):
    return pltpu.roll(value, N // 2, 1) * sign


def y_matmul(rows, table):
    high, low = split(rows)
    both = dot(jnp.concatenate([high, low], axis=1), table)
    return both[:, :N] + both[:, N:]


def x_matmul(table, first, second, upper):
    top = jnp.concatenate([first, second], axis=1)
    below = jnp.concatenate([turned(first, upper), turned(second, upper)], axis=1)
    high, low = split(jnp.concatenate([top, below], axis=0))
    both = dot(table, high)
    result = both[:N] + both[N:] + dot(table[:N], low)
    return result[:, :N], result[:, N:]


def stress_terms(strain, freq_x, freq_y, freq_z):
    xx, yy, zz, yz, xz, xy = strain
    trace = xx + yy + zz
    tau_xx = lame_lambda * trace + 2.0 * shear_modulus * xx
    tau_yy = lame_lambda * trace + 2.0 * shear_modulus * yy
    tau_zz = lame_lambda * trace + 2.0 * shear_modulus * zz
    tau_yz = 2.0 * shear_modulus * yz
    tau_xz = 2.0 * shear_modulus * xz
    tau_xy = 2.0 * shear_modulus * xy
    norm_x = tau_xx * freq_x + tau_xy * freq_y + tau_xz * freq_z
    norm_y = tau_xy * freq_x + tau_yy * freq_y + tau_yz * freq_z
    norm_z = tau_xz * freq_x + tau_yz * freq_y + tau_zz * freq_z
    square = freq_x * freq_x + freq_y * freq_y + freq_z * freq_z
    inverse = 1.0 / jnp.maximum(square, 1.0)
    along = (freq_x * norm_x + freq_y * norm_y + freq_z * norm_z) * inverse * inverse * green_coef
    half = inverse / (2.0 * shear_modulus)

    def term(first_q, second_q, first_n, second_n, plastic):
        total = (first_q * second_n + second_q * first_n) * half - first_q * second_q * along
        return total - plastic

    el_xx = term(freq_x, freq_x, norm_x, norm_x, xx)
    el_yy = term(freq_y, freq_y, norm_y, norm_y, yy)
    el_zz = term(freq_z, freq_z, norm_z, norm_z, zz)
    el_yz = term(freq_y, freq_z, norm_y, norm_z, yz)
    el_xz = term(freq_x, freq_z, norm_x, norm_z, xz)
    el_xy = term(freq_x, freq_y, norm_x, norm_y, xy)
    el_trace = el_xx + el_yy + el_zz
    return (
        lame_lambda * el_trace + 2.0 * shear_modulus * el_xx,
        lame_lambda * el_trace + 2.0 * shear_modulus * el_yy,
        lame_lambda * el_trace + 2.0 * shear_modulus * el_zz,
        2.0 * shear_modulus * el_yz,
        2.0 * shear_modulus * el_xz,
        2.0 * shear_modulus * el_xy,
    )


SEND_COST = ((0.0, 0.6, 1.5, 1.0), (0.0, 1.0, 2.3, 1.6), (0.0, 1.5, 3.6, 2.4))
GREET_COST = ((0.0, 1.0, 2.0, 2.4),) * 3


def partners(cost):
    def distance(i):
        return cost[0][2 * (i >> 6) + (i & 1)] + cost[1][(i & 7) >> 1] + cost[2][(i >> 4) & 3]

    return sorted(range(1, N), key=lambda i: -distance(i))


def signed_frequency(index):
    value = jnp.where(index < N // 2, index, jnp.where(index == N // 2, 0, index - N))
    return value.astype(F32)


def row_of_cells(ref, row, first, count):
    cells, rows = ref.shape[0], ref.shape[1]
    return ref.reshape(cells * rows, N)[pl.ds(first * rows + row, count, stride=rows), :]


def arms_into(mbuf, position, line, burg):
    cells = position[0].shape[0]
    flat = mbuf.reshape(3 * mbuf.shape[1] * 16, N)
    arm = [
        position[1] * line[2] - position[2] * line[1],
        position[2] * line[0] - position[0] * line[2],
        position[0] * line[1] - position[1] * line[0],
    ]
    for shift in range(3):
        moved_arm = [
            arm[0],
            arm[1] - (shift - 1.0) * line[2],
            arm[2] + (shift - 1.0) * line[1],
        ]
        for a in range(3):
            for b in range(3):
                at = shift * mbuf.shape[1] * 16 + 3 * a + b
                flat[pl.ds(at, cells, stride=16), :] = moved_arm[a] * burg[b]


def pair_blocks(position, lbuf, mbuf, pair_out, blocks, before=None):
    cells = position[0].shape[0]
    extra = (WIDE - cells) // 2
    if cells % 8:
        pad = jnp.zeros((16 - cells, N), F32)
        columns = [jnp.transpose(jnp.concatenate([value, pad], axis=0)) for value in position]
    else:
        columns = [jnp.transpose(value) for value in position]
    for cell, shifts in blocks:
        target = [value[cell : cell + 1] for value in position]
        weights, factors = [], []
        for shift in shifts:
            source = cell + shift - 1
            delta = [
                (target[k] - (shift - 1.0) * (k == 0)) - columns[k][:, source : source + 1] for k in range(3)
            ]
            radius = delta[0] * delta[0] + delta[1] * delta[1] + delta[2] * delta[2] + core_square
            root = lax.rsqrt(radius)
            weights.append(root * root * root)
            factors.append(jnp.concatenate([lbuf[source + extra], mbuf[shift, source]], axis=0))
        weight_high, weight_low = split(jnp.concatenate(weights, axis=0))
        factor_high, factor_low = split(jnp.concatenate(factors, axis=1))
        both = dot(jnp.concatenate([factor_high, factor_low], axis=0), weight_high)
        total = both[:32] + both[32:] + dot(factor_high, weight_low)
        if before is not None and len(shifts) < 3:
            total = total + before[cell]
        pair_out[cell] = total


def pair_field(position, pair_out):
    cells = position[0].shape[0]
    spread = [[row_of_cells(pair_out, 3 * c + b, 0, cells) for b in range(3)] for c in range(3)]
    offset = [[row_of_cells(pair_out, 16 + 3 * a + b, 0, cells) for b in range(3)] for a in range(3)]
    moment = [[None] * 3 for _ in range(3)]
    for b in range(3):
        for a in range(3):
            n, m = (a + 1) % 3, (a + 2) % 3
            moment[a][b] = position[n] * spread[m][b] - position[m] * spread[n][b] - offset[a][b]
    return [
        pair_factor * (moment[a][b] + moment[b][a])
        for a, b in ((0, 0), (1, 1), (2, 2), (1, 2), (0, 2), (0, 1))
    ]


def advance(position, sampled, field, line, burg):
    sigma = [sampled[c] + field[c] for c in range(6)]
    pull = [sum(sigma[full_index[a][b]] * burg[b] for b in range(3)) for a in range(3)]
    force = [
        pull[1] * line[2] - pull[2] * line[1],
        pull[2] * line[0] - pull[0] * line[2],
        pull[0] * line[1] - pull[1] * line[0],
    ]
    return [position[k] + step_size * force[k] for k in range(3)]


def kernel(
    plastic_hbm, table_hbm, back_hbm, offsets_hbm, lines_hbm, burgers_hbm, counts_hbm, voxels_hbm,
    stress_out, seg_out, samp_out, field_out, lbuf, second_out, third_out,
    plastic_buf, table_buf, back_buf, offsets_ref, lines_ref, burgers_ref, counts_ref, voxels_ref,
    out1, in1, out2, in2, spec, stress_buf, seg, samp, own, mbuf, mlate, pair_out, factor_buf,
    load_sem, send1, recv1, send2, recv2, halo_send, halo_recv, samp_send, samp_recv,
):
    gx = lax.axis_index("gx")
    pa = lax.axis_index("pa")
    mode = pa * GX + gx
    left = {"gx": (gx + 7) % 8}
    right = {"gx": (gx + 1) % 8}

    def device(i):
        return {"gx": gx ^ (i & 7), "pa": pa ^ (i >> 3)}

    sources = (plastic_hbm, offsets_hbm, lines_hbm, burgers_hbm, counts_hbm, voxels_hbm, back_hbm)
    targets = (plastic_buf, offsets_ref, lines_ref, burgers_ref, counts_ref, voxels_ref, back_buf)
    loads = [
        pltpu.make_async_copy(source, target, load_sem.at[i])
        for i, (source, target) in enumerate(zip(sources, targets))
    ]
    table_loads = [
        pltpu.make_async_copy(table_hbm.at[i], table_buf.at[i], load_sem.at[len(loads) + i]) for i in range(10)
    ]
    barrier = pltpu.get_barrier_semaphore()
    with jax.named_scope("greet"):
        loads[0].start()
        table_loads[0].start()
        table_loads[1].start()
        for i in partners(GREET_COST):
            pl.semaphore_signal(barrier, inc=1, device_id=device(i), device_id_type=MESH)
        for copy in loads[1:] + table_loads[2:]:
            copy.start()

    lane8 = lax.broadcasted_iota(jnp.int32, (8, N), 1)
    upper = jnp.where(lax.broadcasted_iota(jnp.int32, (N, N), 1) >= N // 2, -1.0, 1.0)

    def message(ref, number):
        return ref.at[pl.ds(6 * number, 6)]

    def send_all(source, target, send_sem, recv_sem):
        for i in partners(SEND_COST):
            pltpu.make_async_remote_copy(
                src_ref=message(source, mode ^ i), dst_ref=message(target, mode),
                send_sem=send_sem, recv_sem=recv_sem, device_id=device(i), device_id_type=MESH,
            ).start()
        pltpu.make_async_copy(message(source, mode), message(target, mode), recv_sem).start()

    def wait_all(target, recv_sem):
        pltpu.make_async_copy(target, target, recv_sem).wait()

    def put(target, c, value):
        target[pl.ds(c, N, stride=6), :] = value

    def take(source, c):
        return source[pl.ds(c, N, stride=6), :]

    with jax.named_scope("wait_load"):
        loads[0].wait()
        table_loads[0].wait()
        table_loads[1].wait()
    with jax.named_scope("z_ahead"):
        for pair in PAIRS:
            rows = jnp.concatenate([plastic_buf[c].reshape(N, N) for c in pair], axis=0)
            high, low = split(rows)
            both = dot(table_buf[1 if pair[0] == 3 else 0], jnp.concatenate([high, low], axis=1), (1, 1))
            result = both[:N] + both[N:]
            put(out1, pair[0], result[:, :N])
            put(out1, pair[1], result[:, N:])
    with jax.named_scope("wait_barrier"):
        pl.semaphore_wait(barrier, N - 1)
    with jax.named_scope("send1"):
        send_all(out1, in1, send1, recv1)

    for copy in loads[1:6]:
        copy.wait()
    counts = counts_ref[...]
    index = lax.broadcasted_iota(jnp.int32, (CELLS, N), 1)
    live = (index < counts.reshape(CELLS, 1)).astype(F32)
    first_position = []
    for k in range(3):
        value = offsets_ref[k, 0] - 0.5
        seg[HALO : HALO + CELLS, k, :] = value
        seg[HALO : HALO + CELLS, 3 + k, :] = lines_ref[k, 0]
        seg[HALO : HALO + CELLS, 6 + k, :] = burgers_ref[k, 0] * live
    to_left = pltpu.make_async_remote_copy(
        src_ref=seg.at[pl.ds(HALO, HALO)], dst_ref=seg.at[pl.ds(HALO + CELLS, HALO)],
        send_sem=halo_send.at[0], recv_sem=halo_recv.at[0], device_id=left, device_id_type=MESH,
    )
    to_right = pltpu.make_async_remote_copy(
        src_ref=seg.at[pl.ds(CELLS, HALO)], dst_ref=seg.at[pl.ds(0, HALO)],
        send_sem=halo_send.at[1], recv_sem=halo_recv.at[1], device_id=right, device_id_type=MESH,
    )
    to_left.start()
    to_right.start()

    for copy in table_loads[2:]:
        copy.wait()
    loads[6].wait()
    with jax.named_scope("wait_in1"):
        wait_all(in1, recv1)
    with jax.named_scope("y_ahead"):
        for c in range(6):
            spec[c] = y_matmul(butterfly(take(in1, c), lane8), table_buf[2])
    with jax.named_scope("x_ahead"):
        for pair in PAIRS:
            table = table_buf[4 if pair[0] == 3 else 3]
            spec[pair[0]], spec[pair[1]] = x_matmul(table, spec[pair[0]], spec[pair[1]], upper)

    with jax.named_scope("operator"):
        freq_y = signed_frequency(lane8 % 64)
        freq_z = jnp.where(mode % 2 == 0, mode // 2, -(mode // 2)).astype(F32)
        for t in range(N // 8):
            freq_x = signed_frequency(lax.broadcasted_iota(jnp.int32, (8, N), 0) + 8 * t)
            strain = [spec[c, 8 * t : 8 * t + 8, :] for c in range(6)]
            result = stress_terms(strain, freq_x, freq_y, freq_z)
            for c in range(6):
                spec[c, 8 * t : 8 * t + 8, :] = result[c]

    with jax.named_scope("x_back"):
        for pair in PAIRS:
            table = table_buf[6 if pair[0] == 3 else 5]
            spec[pair[0]], spec[pair[1]] = x_matmul(table, spec[pair[0]], spec[pair[1]], upper)
    with jax.named_scope("y_back"):
        for c in range(6):
            put(out2, c, butterfly(y_matmul(spec[c], table_buf[7]), lane8))
    with jax.named_scope("send2"):
        send_all(out2, in2, send2, recv2)

    with jax.named_scope("wait_halo"):
        to_left.wait()
        to_right.wait()
    start, line, burg = ([row_of_cells(seg, 3 * i + k, 0, WIDE) for k in range(3)] for i in range(3))
    for i, part in enumerate((start, line, burg)):
        for k in range(3):
            seg_out[3 * i + k] = part[k][1 : 1 + LATE]
    with jax.named_scope("pair1"):
        lbuf[...] = jnp.zeros_like(lbuf)
        mbuf[...] = jnp.zeros_like(mbuf)
        mlate[...] = jnp.zeros_like(mlate)
        pair_out[...] = jnp.zeros_like(pair_out)
        own[...] = jnp.zeros_like(own)
        flat = lbuf.reshape(WIDE * 16, N)
        for c in range(3):
            for b in range(3):
                flat[pl.ds(3 * c + b, WIDE, stride=16), :] = line[c] * burg[b]
        arms_into(mbuf, start, line, burg)
        pair_blocks(start, lbuf, mbuf, pair_out, [(cell, (0, 1, 2)) for cell in range(1, WIDE - 1)])
        field = pair_field(start, pair_out)
        for c in range(6):
            field_out[c] = field[c][1 : 1 + LATE]
        second_out[...] = jnp.zeros_like(second_out)
        third_out[...] = jnp.zeros_like(third_out)

    voxels = voxels_ref[0]
    z_of = voxels & 127
    with jax.named_scope("factors"):
        for cell in range(CELLS):
            pick_z = jnp.broadcast_to(z_of[cell : cell + 1], (8, N))
            for odd in range(2):
                for t in range(N // 8):
                    rows = slice(8 * t, 8 * t + 8)
                    factor_buf[cell, odd, rows] = jnp.take_along_axis(
                        back_buf[odd, rows], pick_z, axis=1, mode="promise_in_bounds"
                    )
    with jax.named_scope("wait_in2"):
        wait_all(in2, recv2)
    with jax.named_scope("sample"):
        for c in range(6):
            stress_buf[c] = take(in2, c)
        near_side = gx % 2
        first = 2 * near_side
        far_slot = HALO + CELLS - (HALO + CELLS - 1) * near_side
        copies = []
        for half in range(2):
            begin = first if half == 0 else 2 - first
            for k in range(2):
                cell = begin + k
                pick = jnp.broadcast_to(voxels_ref[0, pl.ds(cell, 1), :] >> 7, (8, N))
                total = [None] * 6
                for t in range(N // 8):
                    rows = slice(8 * t, 8 * t + 8)
                    factor = [factor_buf[cell, odd, rows] for odd in range(2)]
                    for c in range(6):
                        tile = jnp.take_along_axis(stress_buf[c, rows], pick, axis=1, mode="promise_in_bounds")
                        term = tile * factor[1 if c in (3, 4) else 0]
                        total[c] = term if t == 0 else total[c] + term
                for c in range(6):
                    value = jnp.sum(total[c], axis=0, keepdims=True)
                    samp[HALO + cell, c : c + 1, :] = value
                    own[HALO + cell, c : c + 1, :] = value
            other = (gx + 7 + 2 * near_side) % 8 if half == 0 else gx + 1 - 2 * near_side
            slot = far_slot if half == 0 else HALO + CELLS + 1 - far_slot
            copy = pltpu.make_async_remote_copy(
                src_ref=samp.at[pl.ds(HALO + begin, 2)], dst_ref=samp.at[pl.ds(slot, 2)],
                send_sem=samp_send.at[half], recv_sem=samp_recv.at[half], device_id={"gx": other}, device_id_type=MESH,
            )
            copy.start()
            copies.append(copy)
    with jax.named_scope("z_back"):
        for pair in PAIRS:
            table = table_buf[9 if pair[0] == 3 else 8]
            high, low = split(jnp.concatenate([stress_buf[c] for c in pair], axis=1))
            both = dot(table, jnp.concatenate([high, low], axis=0))
            result = both[:N] + both[N:]
            for c, half in zip(pair, (result[:, :N], result[:, N:])):
                stress_out[c] = jnp.transpose(half).reshape(16, 8, N)
    with jax.named_scope("pair_own"):
        start, line, burg = ([seg_out[3 * i + k] for k in range(3)] for i in range(3))
        sampled = [row_of_cells(own, c, 1, LATE) for c in range(6)]
        position = advance(start, sampled, [field_out[c] for c in range(6)], line, burg)
        arms_into(mlate, position, line, burg)
        pair_blocks(position, lbuf, mlate, second_out, OWN_SECOND)
        position = advance(position, sampled, pair_field(position, second_out), line, burg)
        arms_into(mlate, position, line, burg)
        pair_blocks(position, lbuf, mlate, third_out, OWN_THIRD)

    with jax.named_scope("wait_samp"):
        for copy in copies:
            copy.wait()
    for c in range(6):
        samp_out[c] = row_of_cells(samp, c, 1, LATE)

    for source, send_sem in ((out1, send1), (out2, send2)):
        sent = source.at[pl.ds(0, 6 * (N - 1))]
        pltpu.make_async_copy(sent, sent, send_sem).wait()


def finish(
    stress_ref, seg, samp, field_ref, lbuf, second, third, stress_hbm, moved_hbm,
    mbuf, second_buf, third_buf, moved_ref, store_sem,
):
    store = pltpu.make_async_copy(stress_ref, stress_hbm, store_sem.at[0])
    store.start()
    start, line, burg = ([seg[3 * i + k] for k in range(3)] for i in range(3))
    sampled = [samp[c] for c in range(6)]
    for cell in (0, 3, 4, 7):
        second_buf[cell] = second[cell]
    for cell in (0, 1, 6, 7):
        third_buf[cell] = third[cell]
    with jax.named_scope("pair_second"):
        position = advance(start, sampled, [field_ref[c] for c in range(6)], line, burg)
        arms_into(mbuf, position, line, burg)
        pair_blocks(position, lbuf, mbuf, second_buf, REST_SECOND, second)
    with jax.named_scope("pair_third"):
        position = advance(position, sampled, pair_field(position, second_buf), line, burg)
        arms_into(mbuf, position, line, burg)
        pair_blocks(position, lbuf, mbuf, third_buf, REST_THIRD, third)
    with jax.named_scope("last"):
        position = advance(position, sampled, pair_field(position, third_buf), line, burg)
        for k in range(3):
            moved_ref[k, 0] = (position[k] - start[k])[2 : 2 + CELLS]
    moved_store = pltpu.make_async_copy(moved_ref, moved_hbm, store_sem.at[1])
    moved_store.start()
    store.wait()
    moved_store.wait()


def body(plastic, offsets, lines, burgers, counts, voxels):
    any_space = pl.BlockSpec(memory_space=pl.ANY)
    dma = pltpu.SemaphoreType.DMA
    group = pltpu.VMEM((6 * N, N), F32)
    vectors = pltpu.VMEM((3, 1, CELLS, N), F32)
    table, back = tables()
    vmem = pl.BlockSpec(memory_space=pltpu.VMEM)
    state = pl.pallas_call(
        kernel,
        out_shape=(
            pltpu.VMEM((6, 16, 8, N), F32),
            pltpu.VMEM((9, LATE, N), F32),
            pltpu.VMEM((6, LATE, N), F32),
            pltpu.VMEM((6, LATE, N), F32),
            pltpu.VMEM((WIDE, 16, N), F32),
            pltpu.VMEM((LATE, 32, N), F32),
            pltpu.VMEM((LATE, 32, N), F32),
        ),
        in_specs=[any_space] * 8,
        out_specs=(vmem,) * 7,
        scratch_shapes=[
            pltpu.VMEM((6, 16, 8, N), F32),
            pltpu.VMEM((10, 2 * N, 2 * N), BF16),
            pltpu.VMEM((2, N, N), F32),
            vectors, vectors, vectors,
            pltpu.VMEM((1, CELLS), jnp.int32),
            pltpu.VMEM((1, CELLS, N), jnp.int32),
            group, group, group, group,
            pltpu.VMEM((6, N, N), F32),
            pltpu.VMEM((6, N, N), F32),
            pltpu.VMEM((WIDE, 16, N), F32),
            pltpu.VMEM((WIDE, 8, N), F32),
            pltpu.VMEM((WIDE, 8, N), F32),
            pltpu.VMEM((3, WIDE, 16, N), F32),
            pltpu.VMEM((3, LATE, 16, N), F32),
            pltpu.VMEM((WIDE, 32, N), F32),
            pltpu.VMEM((CELLS, 2, N, N), F32),
            dma((17,)),
            dma, dma, dma, dma,
            dma((2,)), dma((2,)), dma((2,)), dma((2,)),
        ],
        compiler_params=pltpu.CompilerParams(collective_id=0, has_side_effects=True),
    )(plastic, jnp.asarray(table), jnp.asarray(back), offsets, lines, burgers, counts, voxels)
    return pl.pallas_call(
        finish,
        out_shape=(
            jax.ShapeDtypeStruct((6, 16, 8, N), F32),
            jax.ShapeDtypeStruct((3, 1, CELLS, N), F32),
        ),
        in_specs=[vmem] * 7,
        out_specs=(any_space, any_space),
        scratch_shapes=[
            pltpu.VMEM((3, LATE, 16, N), F32),
            pltpu.VMEM((LATE, 32, N), F32),
            pltpu.VMEM((LATE, 32, N), F32),
            vectors,
            dma((2,)),
        ],
    )(*[pltpu.with_memory_space_constraint(array, pltpu.VMEM) for array in state])


def solution(mesh):
    placed = (
        P(None, "gx", "pa", None),
        P(None, "pa", "gx", None),
        P(None, "pa", "gx", None),
        P(None, "pa", "gx", None),
        P("pa", "gx"),
        P("pa", "gx", None),
    )
    return jax.shard_map(
        body,
        mesh=mesh,
        in_specs=placed,
        out_specs=(P(None, "gx", "pa", None), P(None, "pa", "gx", None)),
        check_vma=False,
    )
```
